32 devices in a mesh: col: 4 (over z), row: 2 (over y), depth: 4 (over x, core).
Axes of the slice: x: 2, y: 2, z: 4, core: 2. Of those that a mesh axis runs over, the one named last changes fastest.
Arguments:
- a_mat: bfloat16 [4096, 8192], P(('depth', 'row', 'col'))
- b_mat: bfloat16 [8192, 4608], P(('depth', 'row', 'col'))
Outputs:
- output: bfloat16 [4096, 4608], P(('depth', 'row', 'col'))
All inputs are finite; a program needn't handle non-finite values.
Results may differ from the reference program's by a relative error of at most 0.001.
Values are sent between devices in bfloat16 or wider.
A program may use at most 1 GiB of HBM per device.

```python
import jax
import jax.numpy as jnp

D = 4096
F = 4608
TOKENS = 8192


def setup_inputs(seed: int = 0) -> dict:
    key_a, key_b = jax.random.split(jax.random.key(seed))
    a_vals = jax.random.normal(key_a, (D, TOKENS), jnp.float32)
    b_vals = jax.random.normal(key_b, (TOKENS, F), jnp.float32) * (TOKENS ** -0.5)
    return {"a_mat": a_vals.astype(jnp.bfloat16), "b_mat": b_vals.astype(jnp.bfloat16)}


def reference(a_mat, b_mat):
    product = jnp.dot(a_mat, b_mat, preferred_element_type=jnp.float32)
    return product.astype(jnp.bfloat16)
```

```python
import functools

import jax
import jax.numpy as jnp
from jax import lax
from jax.experimental import pallas as pl
from jax.experimental.pallas import tpu as pltpu
from jax.sharding import PartitionSpec as P

MESH = pl.DeviceIdType.MESH
NC = 256
AHEAD = 2


def kernel(n_cols, a_ref, b_ref, c_ref, abuf, bbuf, pbuf, rbuf, obuf, a_loc, b_loc, a_snd, a_rcv, up_snd, up_rcv, dn_snd, dn_rcv, x_snd, x_rcv, r_snd, r_rcv, o_sem):
    depth, y, z = lax.axis_index("depth"), lax.axis_index("row"), lax.axis_index("col")
    x, core = depth // 2, depth % 2
    n_chunks = n_cols // NC
    rows_a = a_ref.shape[0]
    rows_b = b_ref.shape[0]
    half = 4 * rows_b

    up = (z + 1, y, depth)
    down = (z - 1, y, depth)
    twin = (z, y, 2 * x + 1 - core)
    x_peer = (z, y, 2 * (1 - x) + core)
    y_peer = (z, 1 - y, depth)
    diag = (z, 1 - y, 2 * (1 - x) + core)
    plane = (x_peer, y_peer, diag)
    plane_xy = ((1 - x, y), (x, 1 - y), (1 - x, 1 - y))

    def cols(j):
        return pl.ds(pl.multiple_of(j * NC, NC), NC)

    own_rows = pl.ds(pl.multiple_of(core * half + z * rows_b, rows_b), rows_b)
    load_b = pltpu.make_async_copy(b_ref, bbuf.at[own_rows], b_loc)
    load_b.start()

    def a_cols(px, py, k):
        return pl.ds(pl.multiple_of(((2 * px + k) * 2 + py) * half, half), half)

    my_group = pl.ds(pl.multiple_of((2 * x + y) * rows_a, rows_a), rows_a)
    load_a = []
    for k in range(2):
        load_a.append(pltpu.make_async_copy(a_ref.at[:, a_cols(x, y, k)], abuf.at[my_group, pl.ds(k * half, half)], a_loc.at[k]))
        load_a[-1].start()

    barrier = pltpu.get_barrier_semaphore()
    for peer in plane + (twin,):
        pl.semaphore_signal(barrier, inc=1, device_id=peer, device_id_type=MESH)

    @pl.when(z < 3)
    def _():
        pl.semaphore_signal(barrier, inc=1, device_id=up, device_id_type=MESH)

    @pl.when(z > 0)
    def _():
        pl.semaphore_signal(barrier, inc=1, device_id=down, device_id_type=MESH)

    @pl.when((z > 0) & (z < 3))
    def _():
        pl.semaphore_wait(barrier, 6)

    @pl.when((z == 0) | (z == 3))
    def _():
        pl.semaphore_wait(barrier, 5)

    def a_copy(i, k):
        px, py = plane_xy[i]
        return pltpu.make_async_remote_copy(
            a_ref.at[:, a_cols(px, py, k)], abuf.at[my_group, pl.ds(k * half, half)],
            a_snd.at[2 * i + k], a_rcv.at[2 * i + k], device_id=plane[i], device_id_type=MESH)

    def z_copy(h, j, target, snd, rcv, src):
        rows = pl.ds(pl.multiple_of(core * half + src * rows_b, rows_b), rows_b)
        return pltpu.make_async_remote_copy(
            bbuf.at[rows, cols(j)], bbuf.at[rows, cols(j)],
            snd.at[h, j], rcv.at[h, j], device_id=target, device_id_type=MESH)

    def up_send(h, j):
        return z_copy(h, j, up, up_snd, up_rcv, z - h)

    def up_recv(h, j):
        return z_copy(h, j, up, up_snd, up_rcv, z - 1 - h)

    def dn_send(h, j):
        return z_copy(h, j, down, dn_snd, dn_rcv, z + h)

    def dn_recv(h, j):
        return z_copy(h, j, down, dn_snd, dn_rcv, z + 1 + h)

    def twin_copy(j, who):
        rows = pl.ds(pl.multiple_of(who * half, half), half)
        return pltpu.make_async_remote_copy(
            bbuf.at[rows, cols(j)], bbuf.at[rows, cols(j)],
            x_snd.at[j], x_rcv.at[j], device_id=twin, device_id_type=MESH)

    def r_copy(i, j):
        px, py = plane_xy[i]
        return pltpu.make_async_remote_copy(
            pbuf.at[pl.ds(pl.multiple_of((2 * px + py) * rows_a, rows_a), rows_a), cols(j)], rbuf.at[i, :, cols(j)],
            r_snd.at[i, j], r_rcv.at[i, j], device_id=plane[i], device_id_type=MESH)

    def o_copy(j):
        return pltpu.make_async_copy(obuf.at[:, cols(j)], c_ref.at[:, cols(j)], o_sem.at[j])

    def send_own(j):
        @pl.when(z < 3)
        def _():
            up_send(0, j).start()

        @pl.when(z > 0)
        def _():
            dn_send(0, j).start()

    def relay(h, j):
        @pl.when(z >= h)
        def _():
            up_recv(h - 1, j).wait_recv()

        if h < 3:
            @pl.when((z >= h) & (z < 3))
            def _():
                up_send(h, j).start()

        @pl.when(z <= 3 - h)
        def _():
            dn_recv(h - 1, j).wait_recv()

        if h < 3:
            @pl.when((z <= 3 - h) & (z > 0))
            def _():
                dn_send(h, j).start()

    load_b.wait()
    for j in range(AHEAD):
        send_own(j)
    for i in range(3):
        for k in range(2):
            a_copy(i, k).start()

    def guarded(j, fn):
        @pl.when((j >= 0) & (j < n_chunks))
        def _():
            fn(j)

    def last_hop(j):
        relay(3, j)
        twin_copy(j, core).start()

    def multiply(j):
        @pl.when(j == 0)
        def _():
            for k in range(2):
                load_a[k].wait()
            for i in range(3):
                for k in range(2):
                    a_copy(i, k).wait_recv()

        twin_copy(j, 1 - core).wait_recv()
        pbuf[:, cols(j)] = jnp.dot(abuf[...], bbuf[:, cols(j)], preferred_element_type=jnp.float32)
        for i in (2, 0, 1):
            r_copy(i, j).start()

    def finish(j):
        for i in range(3):
            r_copy(i, j).wait_recv()
        total = pbuf[my_group, cols(j)] + rbuf[0, :, cols(j)] + rbuf[1, :, cols(j)] + rbuf[2, :, cols(j)]
        obuf[:, cols(j)] = total.astype(jnp.bfloat16)
        o_copy(j).start()

    @pl.loop(0, n_chunks + 5)
    def _(t):
        guarded(t + AHEAD, send_own)
        guarded(t, functools.partial(relay, 1))
        guarded(t - 1, functools.partial(relay, 2))
        guarded(t - 2, last_hop)
        guarded(t - 3, multiply)
        guarded(t - 5, finish)

    for i in range(3):
        for k in range(2):
            a_copy(i, k).wait_send()

    @pl.loop(0, n_chunks)
    def _(j):
        for h in range(3):
            @pl.when((z >= h) & (z < 3))
            def _():
                up_send(h, j).wait_send()

            @pl.when((z <= 3 - h) & (z > 0))
            def _():
                dn_send(h, j).wait_send()
        twin_copy(j, core).wait_send()
        for i in range(3):
            r_copy(i, j).wait_send()
        o_copy(j).wait()


def solution(mesh):
    all_axes = ("depth", "row", "col")

    def device_block(a_rows, b_rows):
        rows, depth = a_rows.shape
        rows_b, n_cols = b_rows.shape
        n = n_cols // NC
        dma = pltpu.SemaphoreType.DMA
        return pl.pallas_call(
            functools.partial(kernel, n_cols),
            out_shape=jax.ShapeDtypeStruct((rows, n_cols), jnp.bfloat16),
            in_specs=[pl.BlockSpec(memory_space=pl.ANY)] * 2,
            out_specs=pl.BlockSpec(memory_space=pl.ANY),
            scratch_shapes=[
                pltpu.VMEM((4 * rows, 8 * rows_b), jnp.bfloat16),
                pltpu.VMEM((8 * rows_b, n_cols), jnp.bfloat16),
                pltpu.VMEM((4 * rows, n_cols), jnp.float32),
                pltpu.VMEM((3, rows, n_cols), jnp.float32),
                pltpu.VMEM((rows, n_cols), jnp.bfloat16),
                dma((2,)), dma,
                dma((6,)), dma((6,)),
                dma((3, n)), dma((3, n)),
                dma((3, n)), dma((3, n)),
                dma((n,)), dma((n,)),
                dma((3, n)), dma((3, n)),
                dma((n,)),
            ],
            compiler_params=pltpu.CompilerParams(collective_id=0, has_side_effects=True, vmem_limit_bytes=62 * 2**20),
            name="product",
        )(a_rows, b_rows)

    return jax.shard_map(device_block, mesh=mesh, in_specs=(P(all_axes, None), P(all_axes, None)), out_specs=P(all_axes, None), check_vma=False)
```

```python
import functools

import jax
import jax.numpy as jnp
from jax import lax
from jax.experimental import pallas as pl
from jax.experimental.pallas import tpu as pltpu
from jax.sharding import PartitionSpec as P

MESH = pl.DeviceIdType.MESH
NC = 256
PERIOD = 4
JOBS = 4
FIRST_JOB = 12
AHEAD = 3
AHEAD_END = 6
LAG_MULTIPLY, LAG_MIDDLE, LAG_FINISH = 3, 4, 5


def kernel(
    n_cols, a_ref, b_ref, c_ref,
    abuf, abuf2, bbuf, pbuf, rx, ry, sx, sy, pbuf2, rx2, ry2, sx2, sy2, cbuf, obuf,
    a_loc, b_loc, a_snd, a_rcv, a2_snd, a2_rcv, up_snd, up_rcv, dn_snd, dn_rcv, t_snd, t_rcv,
    r_snd, r_rcv, q_snd, q_rcv, c_snd, c_rcv, o_sem,
):
    depth, y, z = lax.axis_index("depth"), lax.axis_index("row"), lax.axis_index("col")
    x, core = depth // 2, depth % 2
    n_chunks = n_cols // NC
    rows_a = a_ref.shape[0]
    rows_b = b_ref.shape[0]
    half = 4 * rows_b
    hr = rows_a // 2
    f32 = jnp.float32

    inner = (z == 1) | (z == 2)
    end = (z == 0) | (z == 3)
    up = (z + 1, y, depth)
    down = (z - 1, y, depth)
    partner = (z + 1 - 2 * (z % 2), y, depth)
    twin = (z, y, 2 * x + 1 - core)
    x_peer = (z, y, 2 * (1 - x) + core)
    y_peer = (z, 1 - y, depth)
    diag = (z, 1 - y, 2 * (1 - x) + core)
    plane = (x_peer, y_peer, diag)
    plane_xy = ((1 - x, y), (x, 1 - y), (1 - x, 1 - y))

    def cols(j):
        return pl.ds(pl.multiple_of(j * NC, NC), NC)

    def job_chunk(i):
        return PERIOD * i + PERIOD - 1

    def shared(j):
        return (j % PERIOD == PERIOD - 1) & (j < PERIOD * JOBS)

    def when(*conds):
        both = conds[0]
        for c in conds[1:]:
            both = both & c
        return pl.when(both)

    own_rows = pl.ds(pl.multiple_of(core * half + z * rows_b, rows_b), rows_b)
    load_b = pltpu.make_async_copy(b_ref, bbuf.at[own_rows], b_loc)
    load_b.start()

    def a_cols(px, py, k):
        return pl.ds(pl.multiple_of(((2 * px + k) * 2 + py) * half, half), half)

    my_group = pl.ds(pl.multiple_of((2 * x + y) * rows_a, rows_a), rows_a)
    load_a = []
    for k in range(2):
        load_a.append(pltpu.make_async_copy(a_ref.at[:, a_cols(x, y, k)], abuf.at[my_group, pl.ds(k * half, half)], a_loc.at[k]))
        load_a[-1].start()

    barrier = pltpu.get_barrier_semaphore()
    for peer in plane + (twin,):
        pl.semaphore_signal(barrier, inc=1, device_id=peer, device_id_type=MESH)

    @when(z < 3)
    def _():
        pl.semaphore_signal(barrier, inc=1, device_id=up, device_id_type=MESH)

    @when(z > 0)
    def _():
        pl.semaphore_signal(barrier, inc=1, device_id=down, device_id_type=MESH)

    @when(inner)
    def _():
        pl.semaphore_wait(barrier, 6)

    @when(end)
    def _():
        pl.semaphore_wait(barrier, 5)

    def remote(src, dst, snd, rcv, target):
        return pltpu.make_async_remote_copy(src, dst, snd, rcv, device_id=target, device_id_type=MESH)

    def a_copy(i, k):
        px, py = plane_xy[i]
        return remote(a_ref.at[:, a_cols(px, py, k)], abuf.at[my_group, pl.ds(k * half, half)], a_snd.at[2 * i + k], a_rcv.at[2 * i + k], plane[i])

    def a2_copy(i):
        rows = pl.ds(pl.multiple_of(i * rows_a, rows_a), rows_a)
        return remote(abuf.at[rows], abuf2.at[rows], a2_snd.at[i], a2_rcv.at[i], partner)

    def z_copy(h, j, target, snd, rcv, src):
        rows = pl.ds(pl.multiple_of(core * half + src * rows_b, rows_b), rows_b)
        return remote(bbuf.at[rows, cols(j)], bbuf.at[rows, cols(j)], snd.at[h, j], rcv.at[h, j], target)

    def up_send(h, j):
        return z_copy(h, j, up, up_snd, up_rcv, z - h)

    def up_recv(h, j):
        return z_copy(h, j, up, up_snd, up_rcv, z - 1 - h)

    def dn_send(h, j):
        return z_copy(h, j, down, dn_snd, dn_rcv, z + h)

    def dn_recv(h, j):
        return z_copy(h, j, down, dn_snd, dn_rcv, z + 1 + h)

    def sends_up(h, j):
        return (z >= h) & ((z < 2) | ((z == 2) & ~shared(j)))

    def sends_dn(h, j):
        return (z <= 3 - h) & ((z > 1) | ((z == 1) & ~shared(j)))

    def gets_up(h, j):
        return (z > h) & ((z < 3) | ~shared(j))

    def gets_dn(h, j):
        return (z < 3 - h) & ((z > 0) | ~shared(j))

    def works(j):
        return inner | ~shared(j)

    def twin_copy(j, who):
        rows = pl.ds(pl.multiple_of(who * half, half), half)
        return remote(bbuf.at[rows, cols(j)], bbuf.at[rows, cols(j)], t_snd.at[j], t_rcv.at[j], twin)

    low, high = pl.ds(0, hr), pl.ds(hr, hr)

    def stage1(own, s, j):
        p, bx, by = (pbuf, rx, ry) if own else (pbuf2, rx2, ry2)
        cs = cols(j)
        return (
            remote(p.at[1 - x, :, low, cs], bx.at[:, :, cs], r_snd.at[0, s], r_rcv.at[0, s], x_peer),
            remote(p.at[:, 1 - y, high, cs], by.at[:, :, cs], r_snd.at[1, s], r_rcv.at[1, s], y_peer),
        )

    def stage2(own, s, j):
        p, bx, by = (pbuf, sx, sy) if own else (pbuf2, sx2, sy2)
        cs = cols(j)
        return (
            remote(p.at[x, 1 - y, low, cs], by.at[:, cs], q_snd.at[0, s], q_rcv.at[0, s], y_peer),
            remote(p.at[1 - x, y, high, cs], bx.at[:, cs], q_snd.at[1, s], q_rcv.at[1, s], x_peer),
        )

    def partial(own, s, j, src):
        a, p = (abuf, pbuf) if own else (abuf2, pbuf2)
        cs = cols(j)
        p[:, :, :, cs] = jnp.dot(a[...], bbuf[:, cols(src)], preferred_element_type=f32).reshape(2, 2, rows_a, NC)
        for c in stage1(own, s, j):
            c.start()

    def middle(own, s, j):
        p, bx, by = (pbuf, rx, ry) if own else (pbuf2, rx2, ry2)
        cs = cols(j)
        one, two = stage1(own, s, j)
        fwd_y, fwd_x = stage2(own, s, j)
        one.wait_recv()
        p[x, 1 - y, low, cs] += bx[1 - y, :, cs]
        fwd_y.start()
        two.wait_recv()
        p[1 - x, y, high, cs] += by[1 - x, :, cs]
        fwd_x.start()

    def finish(own, s, j, dst):
        p, bx, by, qx, qy = (pbuf, rx, ry, sx, sy) if own else (pbuf2, rx2, ry2, sx2, sy2)
        out = obuf if own else cbuf
        cs = cols(j)
        for c in stage2(own, s, j):
            c.wait_recv()
        out[low, cs] = (p[x, y, low, cs] + bx[y, :, cs] + qy[:, cs]).astype(out.dtype)
        out[high, cs] = (p[x, y, high, cs] + by[x, :, cs] + qx[:, cs]).astype(out.dtype)

    def o_copy(j):
        return pltpu.make_async_copy(obuf.at[:, cols(j)], c_ref.at[:, cols(j)], o_sem.at[j])

    def c_copy(i):
        return remote(cbuf.at[:, cols(i)], obuf.at[:, cols(job_chunk(i))], c_snd.at[i], c_rcv.at[i], partner)

    def send_own(j):
        @when(sends_up(0, j))
        def _():
            up_send(0, j).start()

        @when(sends_dn(0, j))
        def _():
            dn_send(0, j).start()

    def relay(h, j):
        @when(gets_up(h - 1, j))
        def _():
            up_recv(h - 1, j).wait_recv()

        if h < 3:
            @when(sends_up(h, j))
            def _():
                up_send(h, j).start()

        @when(gets_dn(h - 1, j))
        def _():
            dn_recv(h - 1, j).wait_recv()

        if h < 3:
            @when(sends_dn(h, j))
            def _():
                dn_send(h, j).start()

    load_b.wait()
    for i in range(3):
        for k in range(2):
            a_copy(i, k).start()
    for j in range(AHEAD_END):
        when(end if j >= AHEAD else (z >= 0))(functools.partial(send_own, j))

    def in_range(j, count, fn, *more):
        when((j >= 0) & (j < count), *more)(lambda: fn(j))

    def last_hop(j):
        relay(3, j)

        @when(works(j))
        def _():
            twin_copy(j, core).start()

    def multiply(j):
        @when(j == 0)
        def _():
            for k in range(2):
                load_a[k].wait()
            for i in range(3):
                for k in range(2):
                    a_copy(i, k).wait_recv()

        @when(end, j < 4)
        def _():
            a2_copy(j).start()

        @when(works(j))
        def _():
            twin_copy(j, 1 - core).wait_recv()
            partial(True, j, j, j)

    def own_middle(j):
        when(works(j))(lambda: middle(True, j, j))

    def own_finish(j):
        @when(works(j))
        def _():
            finish(True, j, j, j)
            o_copy(j).start()

    def job_multiply(i):
        @when(i == 0)
        def _():
            for k in range(4):
                a2_copy(k).wait_recv()

        partial(False, n_chunks + i, i, job_chunk(i))

    def job_middle(i):
        middle(False, n_chunks + i, i)

    def job_finish(i):
        finish(False, n_chunks + i, i, i)
        c_copy(i).start()

    @pl.loop(0, n_chunks + LAG_FINISH)
    def _(t):
        in_range(t + AHEAD, n_chunks, send_own, inner)
        in_range(t + AHEAD_END, n_chunks, send_own, end)
        in_range(t, n_chunks, functools.partial(relay, 1))
        in_range(t - 1, n_chunks, functools.partial(relay, 2))
        in_range(t - 2, n_chunks, last_hop)
        in_range(t - LAG_MULTIPLY, n_chunks, multiply)
        in_range(t - LAG_MULTIPLY - FIRST_JOB, JOBS, job_multiply, inner)
        in_range(t - LAG_MIDDLE, n_chunks, own_middle)
        in_range(t - LAG_MIDDLE - FIRST_JOB, JOBS, job_middle, inner)
        in_range(t - LAG_FINISH, n_chunks, own_finish)
        in_range(t - LAG_FINISH - FIRST_JOB, JOBS, job_finish, inner)

    for i in range(3):
        for k in range(2):
            a_copy(i, k).wait_send()

    @when(end)
    def _():
        @pl.loop(0, JOBS)
        def _(i):
            c_copy(i).wait_recv()
            o_copy(job_chunk(i)).start()

        for i in range(4):
            a2_copy(i).wait_send()

    @when(inner)
    def _():
        @pl.loop(0, JOBS)
        def _(i):
            c_copy(i).wait_send()
            for c in stage1(False, n_chunks + i, i) + stage2(False, n_chunks + i, i):
                c.wait_send()

    @pl.loop(0, n_chunks)
    def _(j):
        for h in range(3):
            @when(sends_up(h, j))
            def _():
                up_send(h, j).wait_send()

            @when(sends_dn(h, j))
            def _():
                dn_send(h, j).wait_send()

        @when(works(j))
        def _():
            twin_copy(j, core).wait_send()
            for c in stage1(True, j, j) + stage2(True, j, j):
                c.wait_send()

        o_copy(j).wait()


def solution(mesh):
    all_axes = ("depth", "row", "col")

    def device_block(a_rows, b_rows):
        rows, depth = a_rows.shape
        rows_b, n_cols = b_rows.shape
        n = n_cols // NC
        hr = rows // 2
        nj = JOBS * NC
        dma = pltpu.SemaphoreType.DMA
        bf16, f32 = jnp.bfloat16, jnp.float32
        return pl.pallas_call(
            functools.partial(kernel, n_cols),
            out_shape=jax.ShapeDtypeStruct((rows, n_cols), bf16),
            in_specs=[pl.BlockSpec(memory_space=pl.ANY)] * 2,
            out_specs=pl.BlockSpec(memory_space=pl.ANY),
            scratch_shapes=[
                pltpu.VMEM((4 * rows, 8 * rows_b), bf16),
                pltpu.VMEM((4 * rows, 8 * rows_b), bf16),
                pltpu.VMEM((8 * rows_b, n_cols), bf16),
                pltpu.VMEM((2, 2, rows, n_cols), f32),
                pltpu.VMEM((2, hr, n_cols), f32), pltpu.VMEM((2, hr, n_cols), f32),
                pltpu.VMEM((hr, n_cols), f32), pltpu.VMEM((hr, n_cols), f32),
                pltpu.VMEM((2, 2, rows, nj), f32),
                pltpu.VMEM((2, hr, nj), f32), pltpu.VMEM((2, hr, nj), f32),
                pltpu.VMEM((hr, nj), f32), pltpu.VMEM((hr, nj), f32),
                pltpu.VMEM((rows, nj), bf16),
                pltpu.VMEM((rows, n_cols), bf16),
                dma((2,)), dma,
                dma((6,)), dma((6,)), dma((4,)), dma((4,)),
                dma((3, n)), dma((3, n)),
                dma((3, n)), dma((3, n)),
                dma((n,)), dma((n,)),
                dma((2, n + JOBS)), dma((2, n + JOBS)),
                dma((2, n + JOBS)), dma((2, n + JOBS)),
                dma((JOBS,)), dma((JOBS,)),
                dma((n,)),
            ],
            compiler_params=pltpu.CompilerParams(collective_id=0, has_side_effects=True, vmem_limit_bytes=62 * 2**20),
            name="product",
        )(a_rows, b_rows)

    return jax.shard_map(device_block, mesh=mesh, in_specs=(P(all_axes, None), P(all_axes, None)), out_specs=P(all_axes, None), check_vma=False)
```

```python
import functools

import jax
import jax.numpy as jnp
from jax import lax
from jax.experimental import pallas as pl
from jax.experimental.pallas import tpu as pltpu
from jax.sharding import PartitionSpec as P

MESH = pl.DeviceIdType.MESH
NC = 256
SHARED = 5
JOBS = 4
FIRST_JOB, JOB_PERIOD = 4, 3
AHEAD = 3
AHEAD_END = 5
A2_FIRST = 3
A2_STEPS = {5: 4, 7: 5, 9: 6, 11: 7}
LAG_MULTIPLY, LAG_MIDDLE, LAG_FINISH = 1, 1, 2
LAG_JOB_MIDDLE, LAG_JOB_FINISH = 2, 4
RING_Z, RING = 8, 4


def kernel(
    n_cols, a_ref, b_ref, c_ref,
    abuf, abuf2, bbuf, pbuf, rx, ry, sx, sy, pbuf2, rx2, ry2, sx2, sy2, cbuf, obuf,
    loc, a_rcv, a2_rcv, up0_rcv, dn0_rcv, out_rcv, up_rcv, dn_rcv, t_rcv, r_rcv, q_rcv, rj_rcv, qj_rcv, c_rcv,
    a_snd, a2_snd, up_snd, dn_snd, t_snd, r_snd, q_snd, rj_snd, qj_snd, c_snd, o_sem,
):
    depth, y, z = lax.axis_index("depth"), lax.axis_index("row"), lax.axis_index("col")
    x, core = depth // 2, depth % 2
    n_chunks = n_cols // NC
    rows_a = a_ref.shape[0]
    rows_b = b_ref.shape[0]
    half = 4 * rows_b
    hr = rows_a // 2
    jr = rows_a // JOBS
    f32 = jnp.float32
    wide = SHARED * NC

    inner = (z == 1) | (z == 2)
    end = (z == 0) | (z == 3)
    up = (z + 1, y, depth)
    down = (z - 1, y, depth)
    partner = (z + 1 - 2 * (z % 2), y, depth)
    twin = (z, y, 2 * x + 1 - core)
    x_peer = (z, y, 2 * (1 - x) + core)
    y_peer = (z, 1 - y, depth)
    diag = (z, 1 - y, 2 * (1 - x) + core)
    plane = (x_peer, y_peer, diag)
    plane_xy = ((1 - x, y), (x, 1 - y), (1 - x, 1 - y))

    def cols(j):
        return pl.ds(pl.multiple_of(j * NC, NC), NC)

    all_cols = pl.ds(0, n_cols)
    rest_cols = pl.ds(wide, n_cols - wide)

    def shared(j):
        return j < SHARED

    def works(j):
        return inner | ~shared(j)

    def when(*conds):
        both = conds[0]
        for c in conds[1:]:
            both = both & c
        return pl.when(both)

    def b_rows(src):
        return pl.ds(pl.multiple_of(core * half + src * rows_b, rows_b), rows_b)

    def a_cols(px, py, k):
        return pl.ds(pl.multiple_of(((2 * px + k) * 2 + py) * half, half), half)

    load_b = pltpu.make_async_copy(b_ref, bbuf.at[b_rows(z)], loc.at[0])
    load_b.start()
    load_a = []
    for k in range(2):
        load_a.append(pltpu.make_async_copy(a_ref.at[:, a_cols(x, y, k)], abuf.at[2 * x + y, :, pl.ds(k * half, half)], loc.at[1 + k]))
        load_a[-1].start()

    barrier = pltpu.get_barrier_semaphore()
    for peer in plane + (twin,):
        pl.semaphore_signal(barrier, inc=1, device_id=peer, device_id_type=MESH)

    @when(z < 3)
    def _():
        pl.semaphore_signal(barrier, inc=1, device_id=up, device_id_type=MESH)

    @when(z > 0)
    def _():
        pl.semaphore_signal(barrier, inc=1, device_id=down, device_id_type=MESH)

    @when(inner)
    def _():
        pl.semaphore_wait(barrier, 6)

    @when(end)
    def _():
        pl.semaphore_wait(barrier, 5)

    def remote(src, dst, snd, rcv, target):
        return pltpu.make_async_remote_copy(src, dst, snd, rcv, device_id=target, device_id_type=MESH)

    def await_sent(ref, sem):
        remote(ref, ref, sem, loc.at[0], twin).wait_send()

    def await_got(ref, sem):
        remote(ref, ref, loc.at[0], sem, twin).wait_recv()

    def a_copy(i, k):
        px, py = plane_xy[i]
        return remote(a_ref.at[:, a_cols(px, py, k)], abuf.at[2 * x + y, :, pl.ds(k * half, half)], a_snd.at[0], a_rcv.at[0], plane[i])

    def get_a():
        await_got(abuf.at[pl.ds(0, 3)], a_rcv.at[0])

    def job_rows(i):
        return pl.ds(pl.multiple_of(i * jr, jr), jr)

    def a2_copy(i):
        part = jr // 2
        rows = pl.ds(pl.multiple_of(i * part, part), part)
        return remote(abuf.at[:, rows], abuf2.at[:, rows], a2_snd.at[0], a2_rcv.at[i // 2], partner)

    def z_copy(j, src, snd, rcv, target):
        return remote(bbuf.at[b_rows(src), cols(j)], bbuf.at[b_rows(src), cols(j)], snd, rcv, target)

    def up_copy(h, j, src):
        return z_copy(j, src, up_snd.at[h], up0_rcv.at[j] if h == 0 else up_rcv.at[h - 1, j % RING_Z], up)

    def dn_copy(h, j, src):
        return z_copy(j, src, dn_snd.at[h], dn0_rcv.at[j] if h == 0 else dn_rcv.at[h - 1, j % RING_Z], down)

    def outward(src, snd, target):
        return remote(bbuf.at[b_rows(src), rest_cols], bbuf.at[b_rows(src), rest_cols], snd, out_rcv.at[0], target)

    def send_inward(j):
        @when(z < 2)
        def _():
            up_copy(0, j, z).start()

        @when(z > 1)
        def _():
            dn_copy(0, j, z).start()

    def relay(h, j):
        if h == 1:
            @when(inner)
            def _():
                up_copy(0, j, z - 1).wait_recv()

            @when(z == 3, j == SHARED)
            def _():
                outward(z - 1, up_snd.at[0], up).wait_recv()
        else:
            @when(z >= h, (z < 3) | ~shared(j))
            def _():
                up_copy(h - 1, j, z - h).wait_recv()

        if h < 3:
            @when(z >= h, (z < 2) | ((z == 2) & ~shared(j)))
            def _():
                up_copy(h, j, z - h).start()

        if h == 1:
            @when(inner)
            def _():
                dn_copy(0, j, z + 1).wait_recv()

            @when(z == 0, j == SHARED)
            def _():
                outward(z + 1, dn_snd.at[0], down).wait_recv()
        else:
            @when(z <= 3 - h, (z > 0) | ~shared(j))
            def _():
                dn_copy(h - 1, j, z + h).wait_recv()

        if h < 3:
            @when(z <= 3 - h, (z > 1) | ((z == 1) & ~shared(j)))
            def _():
                dn_copy(h, j, z + h).start()

    def twin_copy(j, who):
        rows = pl.ds(pl.multiple_of(who * half, half), half)
        return remote(bbuf.at[rows, cols(j)], bbuf.at[rows, cols(j)], t_snd.at[0], t_rcv.at[j % RING], twin)

    def send_twin(j):
        @when(works(j))
        def _():
            twin_copy(j, core).start()

    def view(own, j):
        if own:
            return pbuf, (rx, ry), (sx, sy), pl.ds(0, hr), pl.ds(hr, hr), pl.ds(0, hr), cols(j)
        lo = pl.multiple_of(j * jr, jr)
        return pbuf2, (rx2, ry2), (sx2, sy2), pl.ds(lo, jr // 2), pl.ds(pl.multiple_of(lo + jr // 2, jr // 2), jr // 2), pl.ds(pl.multiple_of(j * (jr // 2), jr // 2), jr // 2), pl.ds(0, wide)

    def sems(own, j):
        if own:
            return r_snd.at[0], r_rcv.at[j % RING], q_snd.at[0], q_rcv.at[j % RING]
        return rj_snd.at[0], rj_rcv.at[j], qj_snd.at[0], qj_rcv.at[j]

    def first_stage(own, j):
        p, (bx, by), _, low, high, rs, cs = view(own, j)
        snd, rcv, _, _ = sems(own, j)
        remote(p.at[1 - x, :, low, cs], bx.at[:, rs, cs], snd, rcv, x_peer).start()
        remote(p.at[:, 1 - y, high, cs], by.at[:, rs, cs], snd, rcv, y_peer).start()

    def middle(own, j):
        p, (bx, by), (qx, qy), low, high, rs, cs = view(own, j)
        _, got, snd, rcv = sems(own, j)
        await_got(p.at[:, :, low, cs], got)
        p[x, 1 - y, low, cs] += bx[1 - y, rs, cs]
        p[1 - x, y, high, cs] += by[1 - x, rs, cs]
        remote(p.at[x, 1 - y, low, cs], qy.at[rs, cs], snd, rcv, y_peer).start()
        remote(p.at[1 - x, y, high, cs], qx.at[rs, cs], snd, rcv, x_peer).start()

    def finish(own, j):
        p, (bx, by), (qx, qy), low, high, rs, cs = view(own, j)
        out = obuf if own else cbuf
        await_got(p.at[0, :, low, cs], sems(own, j)[3])
        top = p[x, y, low, cs] + bx[y, rs, cs] + qy[rs, cs]
        bottom = p[x, y, high, cs] + by[x, rs, cs] + qx[rs, cs]
        rows = pl.ds(0, rows_a) if own else job_rows(j)
        out[rows, cs] = jnp.concatenate([top, bottom], axis=0).astype(out.dtype)

    def o_copy(cs):
        return pltpu.make_async_copy(obuf.at[:, cs], c_ref.at[:, cs], o_sem.at[0])

    def c_copy(i):
        return remote(cbuf.at[job_rows(i)], obuf.at[job_rows(i), pl.ds(0, wide)], c_snd.at[0], c_rcv.at[0], partner)

    def multiply(j):
        when(inner, j == 0)(get_a)

        @when(works(j))
        def _():
            twin_copy(j, 1 - core).wait_recv()
            a = abuf[...].reshape(4 * rows_a, 2 * half)
            pbuf[:, :, :, cols(j)] = jnp.dot(a, bbuf[:, cols(j)], preferred_element_type=f32).reshape(2, 2, rows_a, NC)
            first_stage(True, j)

    def own_middle(j):
        when(works(j))(lambda: middle(True, j))

    def own_finish(j):
        @when(works(j))
        def _():
            finish(True, j)
            o_copy(cols(j)).start()

    def job_multiply(i):
        await_got(abuf2.at[:, job_rows(i)], a2_rcv.at[i])
        a = abuf2[:, job_rows(i), :].reshape(4 * jr, 2 * half)

        @pl.loop(0, wide // 256)
        def _(j):
            cs = pl.ds(pl.multiple_of(j * 256, 256), 256)
            pbuf2[:, :, job_rows(i), cs] = jnp.dot(a, bbuf[:, cs], preferred_element_type=f32).reshape(2, 2, jr, 256)

        first_stage(False, i)

    def job_middle(i):
        middle(False, i)

    def job_finish(i):
        finish(False, i)
        c_copy(i).start()

    def second_hop(j):
        relay(2, j)
        send_twin(j)

    def third_hop(j):
        relay(3, j)
        send_twin(j)

    def in_range(j, count, fn, *more):
        when((j >= 0) & (j < count), *more)(lambda: fn(j))

    def job(m, fn):
        m = m - FIRST_JOB
        when(inner, m >= 0, m % JOB_PERIOD == 0, m < JOBS * JOB_PERIOD)(lambda: fn(m // JOB_PERIOD))

    load_b.wait()

    @when(inner)
    def _():
        for j in range(AHEAD):
            send_inward(j)

    @when(end)
    def _():
        @pl.loop(0, AHEAD_END)
        def _(j):
            send_inward(j)

    @when(z == 2)
    def _():
        outward(z, up_snd.at[0], up).start()

    @when(z == 1)
    def _():
        outward(z, dn_snd.at[0], down).start()

    for i in range(3):
        for k in range(2):
            a_copy(i, k).start()
    for k in range(2):
        load_a[k].wait()

    @pl.loop(0, n_chunks + 2 + LAG_MULTIPLY + LAG_FINISH)
    def _(t):
        m = t - 2 - LAG_MULTIPLY + (z % 3 + 1) // 2

        @when(end, t == A2_FIRST)
        def _():
            get_a()
            for i in range(4):
                a2_copy(i).start()

        in_range(t + AHEAD, n_chunks, send_inward, inner)
        in_range(t + AHEAD_END, n_chunks, send_inward, end)
        for step, piece in A2_STEPS.items():
            @when(end, t == step)
            def _():
                a2_copy(piece).start()
        in_range(t, n_chunks, functools.partial(relay, 1))
        in_range(t - 1, n_chunks, functools.partial(relay, 2), end)
        in_range(m, n_chunks, multiply)
        job(m, job_multiply)
        in_range(m - LAG_MIDDLE, n_chunks, own_middle)
        job(m - LAG_JOB_MIDDLE, job_middle)
        in_range(m - LAG_FINISH, n_chunks, own_finish)
        job(m - LAG_JOB_FINISH, job_finish)
        in_range(t - 1, n_chunks, second_hop, inner)
        in_range(t - 2, n_chunks, third_hop, end)

    await_sent(abuf.at[pl.ds(0, 3)], a_snd.at[0])

    def sent(cs):
        await_sent(bbuf.at[pl.ds(0, half), cs], t_snd.at[0])
        await_sent(pbuf.at[:, :, pl.ds(0, hr), cs], r_snd.at[0])
        await_sent(pbuf.at[0, :, pl.ds(0, hr), cs], q_snd.at[0])

    def strip(cs):
        return bbuf.at[pl.ds(0, rows_b), cs]

    @when(inner)
    def _():
        sent(all_cols)
        await_sent(pbuf2.at[:, :, pl.ds(0, hr)], rj_snd.at[0])
        await_sent(pbuf2.at[0, :, pl.ds(0, hr)], qj_snd.at[0])
        await_sent(cbuf, c_snd.at[0])

    @when(z == 0)
    def _():
        await_sent(strip(all_cols), up_snd.at[0])

    @when(z == 3)
    def _():
        await_sent(strip(all_cols), dn_snd.at[0])

    @when(z == 1)
    def _():
        for h in range(2):
            await_sent(strip(all_cols), up_snd.at[h])
        for h in range(3):
            await_sent(strip(rest_cols), dn_snd.at[h])

    @when(z == 2)
    def _():
        for h in range(2):
            await_sent(strip(all_cols), dn_snd.at[h])
        for h in range(3):
            await_sent(strip(rest_cols), up_snd.at[h])

    @when(end)
    def _():
        sent(rest_cols)
        await_sent(abuf, a2_snd.at[0])
        await_got(cbuf, c_rcv.at[0])
        o_copy(pl.ds(0, wide)).start()

    o_copy(all_cols).wait()


def solution(mesh):
    all_axes = ("depth", "row", "col")

    def device_block(a_rows, b_rows):
        rows, depth = a_rows.shape
        rows_b, n_cols = b_rows.shape
        n = n_cols // NC
        hr = rows // 2
        nj = SHARED * NC
        dma = pltpu.SemaphoreType.DMA
        bf16, f32 = jnp.bfloat16, jnp.float32
        return pl.pallas_call(
            functools.partial(kernel, n_cols),
            out_shape=jax.ShapeDtypeStruct((rows, n_cols), bf16),
            in_specs=[pl.BlockSpec(memory_space=pl.ANY)] * 2,
            out_specs=pl.BlockSpec(memory_space=pl.ANY),
            scratch_shapes=[
                pltpu.VMEM((4, rows, 8 * rows_b), bf16),
                pltpu.VMEM((4, rows, 8 * rows_b), bf16),
                pltpu.VMEM((8 * rows_b, n_cols), bf16),
                pltpu.VMEM((2, 2, rows, n_cols), f32),
                pltpu.VMEM((2, hr, n_cols), f32), pltpu.VMEM((2, hr, n_cols), f32),
                pltpu.VMEM((hr, n_cols), f32), pltpu.VMEM((hr, n_cols), f32),
                pltpu.VMEM((2, 2, rows, nj), f32),
                pltpu.VMEM((2, hr, nj), f32), pltpu.VMEM((2, hr, nj), f32),
                pltpu.VMEM((hr, nj), f32), pltpu.VMEM((hr, nj), f32),
                pltpu.VMEM((rows, nj), bf16),
                pltpu.VMEM((rows, n_cols), bf16),
                dma((3,)), dma((1,)), dma((JOBS,)),
                dma((n,)), dma((n,)), dma((1,)), dma((2, RING_Z)), dma((2, RING_Z)),
                dma((RING,)), dma((RING,)), dma((RING,)), dma((JOBS,)), dma((JOBS,)), dma((1,)),
                dma((1,)), dma((1,)), dma((3,)), dma((3,)),
                dma((1,)), dma((1,)), dma((1,)), dma((1,)), dma((1,)), dma((1,)), dma((1,)),
            ],
            compiler_params=pltpu.CompilerParams(collective_id=0, has_side_effects=True, vmem_limit_bytes=62 * 2**20),
            name="product",
        )(a_rows, b_rows)

    return jax.shard_map(device_block, mesh=mesh, in_specs=(P(all_axes, None), P(all_axes, None)), out_specs=P(all_axes, None), check_vma=False)
```

```python
import functools

import jax
import jax.numpy as jnp
from jax import lax
from jax.experimental import pallas as pl
from jax.experimental.pallas import tpu as pltpu
from jax.sharding import PartitionSpec as P

MESH = pl.DeviceIdType.MESH
NC = 256
SHARED = 5
JOBS = 4
FIRST_JOB, JOB_PERIOD = 4, 3
AHEAD = 3
AHEAD_END = 5
A2_FIRST = 3
A2_STEPS = {5: 4, 7: 5, 9: 6, 11: 7}
LAG_MULTIPLY = 1
LAG_MIDDLE, LAG_FINISH = (1, 1), (3, 2)
LAG_JOB_MIDDLE, LAG_JOB_FINISH = 2, 4
RING_Z, RING = 12, 8
EXTRA = (9, 12)


def kernel(
    n_cols, a_ref, b_ref, c_ref,
    abuf, abuf2, bbuf, pbuf, rx, ry, sx, sy, pbuf2, rx2, ry2, sx2, sy2, cbuf,
    loc, a_rcv, a2_rcv, up0_rcv, dn0_rcv, out_rcv, up_rcv, dn_rcv, t_rcv, r_rcv, q_rcv, rj_rcv, qj_rcv, c_rcv,
    a_snd, a2_snd, up_snd, dn_snd, t_snd, r_snd, q_snd, rj_snd, qj_snd, c_snd,
):
    depth, y, z = lax.axis_index("depth"), lax.axis_index("row"), lax.axis_index("col")
    x, core = depth // 2, depth % 2
    n_chunks = n_cols // NC
    rows_a = a_ref.shape[0]
    rows_b = b_ref.shape[0]
    half = 4 * rows_b
    hr = rows_a // 2
    jr = rows_a // JOBS
    f32 = jnp.float32
    wide = SHARED * NC

    inner = (z == 1) | (z == 2)
    end = (z == 0) | (z == 3)
    up = (z + 1, y, depth)
    down = (z - 1, y, depth)
    partner = (z + 1 - 2 * (z % 2), y, depth)
    twin = (z, y, 2 * x + 1 - core)
    x_peer = (z, y, 2 * (1 - x) + core)
    y_peer = (z, 1 - y, depth)
    diag = (z, 1 - y, 2 * (1 - x) + core)
    plane = (x_peer, y_peer, diag)
    plane_xy = ((1 - x, y), (x, 1 - y), (1 - x, 1 - y))

    def cols(j):
        return pl.ds(pl.multiple_of(j * NC, NC), NC)

    all_cols = pl.ds(0, n_cols)
    rest_cols = pl.ds(wide, n_cols - wide)

    def shared(j):
        return j < SHARED

    def works(j):
        return inner | ~shared(j)

    def when(*conds):
        both = conds[0]
        for c in conds[1:]:
            both = both & c
        return pl.when(both)

    def b_rows(src):
        return pl.ds(pl.multiple_of(core * half + src * rows_b, rows_b), rows_b)

    def a_cols(px, py, k):
        return pl.ds(pl.multiple_of(((2 * px + k) * 2 + py) * half, half), half)

    load_b = pltpu.make_async_copy(b_ref, bbuf.at[b_rows(z)], loc.at[0])
    load_b.start()
    load_a = []
    for k in range(2):
        load_a.append(pltpu.make_async_copy(a_ref.at[:, a_cols(x, y, k)], abuf.at[2 * x + y, :, pl.ds(k * half, half)], loc.at[1 + k]))
        load_a[-1].start()

    barrier = pltpu.get_barrier_semaphore()
    for peer in plane + (twin,):
        pl.semaphore_signal(barrier, inc=1, device_id=peer, device_id_type=MESH)

    @when(z < 3)
    def _():
        pl.semaphore_signal(barrier, inc=1, device_id=up, device_id_type=MESH)

    @when(z > 0)
    def _():
        pl.semaphore_signal(barrier, inc=1, device_id=down, device_id_type=MESH)

    @when(inner)
    def _():
        pl.semaphore_wait(barrier, 6)

    @when(end)
    def _():
        pl.semaphore_wait(barrier, 5)

    def remote(src, dst, snd, rcv, target):
        return pltpu.make_async_remote_copy(src, dst, snd, rcv, device_id=target, device_id_type=MESH)

    def await_sent(ref, sem):
        remote(ref, ref, sem, loc.at[0], twin).wait_send()

    def await_got(ref, sem):
        remote(ref, ref, loc.at[0], sem, twin).wait_recv()

    def a_copy(i, k):
        px, py = plane_xy[i]
        return remote(a_ref.at[:, a_cols(px, py, k)], abuf.at[2 * x + y, :, pl.ds(k * half, half)], a_snd.at[0], a_rcv.at[0], plane[i])

    def get_a():
        await_got(abuf.at[pl.ds(0, 3)], a_rcv.at[0])

    def job_rows(i):
        return pl.ds(pl.multiple_of(i * jr, jr), jr)

    def a2_copy(i):
        part = jr // 2
        rows = pl.ds(pl.multiple_of(i * part, part), part)
        return remote(abuf.at[:, rows], abuf2.at[:, rows], a2_snd.at[0], a2_rcv.at[i // 2], partner)

    def z_copy(j, src, snd, rcv, target):
        return remote(bbuf.at[b_rows(src), cols(j)], bbuf.at[b_rows(src), cols(j)], snd, rcv, target)

    def up_copy(h, j, src):
        return z_copy(j, src, up_snd.at[h], up0_rcv.at[j] if h == 0 else up_rcv.at[h - 1, j % RING_Z], up)

    def dn_copy(h, j, src):
        return z_copy(j, src, dn_snd.at[h], dn0_rcv.at[j] if h == 0 else dn_rcv.at[h - 1, j % RING_Z], down)

    def outward(src, snd, target):
        return remote(bbuf.at[b_rows(src), rest_cols], bbuf.at[b_rows(src), rest_cols], snd, out_rcv.at[0], target)

    def send_inward(j):
        @when(z < 2)
        def _():
            up_copy(0, j, z).start()

        @when(z > 1)
        def _():
            dn_copy(0, j, z).start()

    def relay(h, j):
        if h == 1:
            @when(inner)
            def _():
                up_copy(0, j, z - 1).wait_recv()

            @when(z == 3, j == SHARED)
            def _():
                outward(z - 1, up_snd.at[0], up).wait_recv()
        else:
            @when(z >= h, (z < 3) | ~shared(j))
            def _():
                up_copy(h - 1, j, z - h).wait_recv()

        if h < 3:
            @when(z >= h, (z < 2) | ((z == 2) & ~shared(j)))
            def _():
                up_copy(h, j, z - h).start()

        if h == 1:
            @when(inner)
            def _():
                dn_copy(0, j, z + 1).wait_recv()

            @when(z == 0, j == SHARED)
            def _():
                outward(z + 1, dn_snd.at[0], down).wait_recv()
        else:
            @when(z <= 3 - h, (z > 0) | ~shared(j))
            def _():
                dn_copy(h - 1, j, z + h).wait_recv()

        if h < 3:
            @when(z <= 3 - h, (z > 1) | ((z == 1) & ~shared(j)))
            def _():
                dn_copy(h, j, z + h).start()

    def twin_copy(j, who):
        rows = pl.ds(pl.multiple_of(who * half, half), half)
        return remote(bbuf.at[rows, cols(j)], bbuf.at[rows, cols(j)], t_snd.at[0], t_rcv.at[j % RING], twin)

    def send_twin(j):
        @when(works(j))
        def _():
            twin_copy(j, core).start()

    def view(own, j):
        if own:
            return pbuf, (rx, ry), (sx, sy), pl.ds(0, hr), pl.ds(hr, hr), pl.ds(0, hr), cols(j)
        lo = pl.multiple_of(j * jr, jr)
        return pbuf2, (rx2, ry2), (sx2, sy2), pl.ds(lo, jr // 2), pl.ds(pl.multiple_of(lo + jr // 2, jr // 2), jr // 2), pl.ds(pl.multiple_of(j * (jr // 2), jr // 2), jr // 2), pl.ds(0, wide)

    def sems(own, j):
        if own:
            return r_snd.at[0], r_rcv.at[j % RING], q_snd.at[0], q_rcv.at[j % RING]
        return rj_snd.at[0], rj_rcv.at[j], qj_snd.at[0], qj_rcv.at[j]

    def first_stage(own, j):
        p, (bx, by), _, low, high, rs, cs = view(own, j)
        snd, rcv, _, _ = sems(own, j)
        remote(p.at[1 - x, :, low, cs], bx.at[:, rs, cs], snd, rcv, x_peer).start()
        remote(p.at[:, 1 - y, high, cs], by.at[:, rs, cs], snd, rcv, y_peer).start()

    def middle(own, j):
        p, (bx, by), (qx, qy), low, high, rs, cs = view(own, j)
        _, got, snd, rcv = sems(own, j)
        await_got(p.at[:, :, low, cs], got)
        p[x, 1 - y, low, cs] += bx[1 - y, rs, cs]
        p[1 - x, y, high, cs] += by[1 - x, rs, cs]
        remote(p.at[x, 1 - y, low, cs], qy.at[rs, cs], snd, rcv, y_peer).start()
        remote(p.at[1 - x, y, high, cs], qx.at[rs, cs], snd, rcv, x_peer).start()

    def finish(own, j):
        p, (bx, by), (qx, qy), low, high, rs, cs = view(own, j)
        out = c_ref if own else cbuf
        await_got(p.at[0, :, low, cs], sems(own, j)[3])
        top = p[x, y, low, cs] + bx[y, rs, cs] + qy[rs, cs]
        bottom = p[x, y, high, cs] + by[x, rs, cs] + qx[rs, cs]
        rows = pl.ds(0, rows_a) if own else job_rows(j)
        out[rows, cs] = jnp.concatenate([top, bottom], axis=0).astype(out.dtype)

    def c_copy(i):
        return remote(cbuf.at[job_rows(i)], c_ref.at[job_rows(i), pl.ds(0, wide)], c_snd.at[0], c_rcv.at[0], partner)

    def multiply(j):
        when(inner, j == 0)(get_a)

        @when(works(j))
        def _():
            twin_copy(j, 1 - core).wait_recv()
            a = abuf[...].reshape(4 * rows_a, 2 * half)
            pbuf[:, :, :, cols(j)] = jnp.dot(a, bbuf[:, cols(j)], preferred_element_type=f32).reshape(2, 2, rows_a, NC)
            first_stage(True, j)

    def own_middle(j):
        when(works(j))(lambda: middle(True, j))

    def own_finish(j):
        @when(works(j))
        def _():
            finish(True, j)

    def job_multiply(i):
        await_got(abuf2.at[:, job_rows(i)], a2_rcv.at[i])
        a = abuf2[:, job_rows(i), :].reshape(4 * jr, 2 * half)

        @pl.loop(0, wide // 256)
        def _(j):
            cs = pl.ds(pl.multiple_of(j * 256, 256), 256)
            pbuf2[:, :, job_rows(i), cs] = jnp.dot(a, bbuf[:, cs], preferred_element_type=f32).reshape(2, 2, jr, 256)

        first_stage(False, i)

    def job_middle(i):
        middle(False, i)

    def job_finish(i):
        finish(False, i)
        c_copy(i).start()

    def second_hop(j):
        relay(2, j)
        send_twin(j)

    def third_hop(j):
        relay(3, j)
        send_twin(j)

    def in_range(j, count, fn, *more):
        when((j >= 0) & (j < count), *more)(lambda: fn(j))

    def job(m, fn):
        m = m - FIRST_JOB
        when(inner, m >= 0, m % JOB_PERIOD == 0, m < JOBS * JOB_PERIOD)(lambda: fn(m // JOB_PERIOD))

    load_b.wait()

    @when(inner)
    def _():
        for j in range(AHEAD):
            send_inward(j)

    @when(end)
    def _():
        @pl.loop(0, AHEAD_END)
        def _(j):
            send_inward(j)

    @when(z == 2)
    def _():
        outward(z, up_snd.at[0], up).start()

    @when(z == 1)
    def _():
        outward(z, dn_snd.at[0], down).start()

    for i in range(3):
        for k in range(2):
            a_copy(i, k).start()
    for k in range(2):
        load_a[k].wait()

    flag = (z % 3 + 1) // 2

    def first_hops(r):
        in_range(r + AHEAD, n_chunks, send_inward, inner)
        in_range(r + AHEAD_END, n_chunks, send_inward, end)
        for step, piece in A2_STEPS.items():
            @when(end, r == step)
            def _():
                a2_copy(piece).start()
        in_range(r, n_chunks, functools.partial(relay, 1))
        in_range(r - 1, n_chunks, functools.partial(relay, 2), end)

    def last_hops(r):
        in_range(r - 1, n_chunks, second_hop, inner)
        in_range(r - 2, n_chunks, third_hop, end)

    def lag(pair):
        return pair[1] + flag * (pair[0] - pair[1])

    @pl.loop(0, n_chunks + 2 + LAG_MULTIPLY + max(LAG_FINISH))
    def _(t):
        m = t - 2 - LAG_MULTIPLY + flag
        r = t
        for e in EXTRA:
            r = r + flag * jnp.where(t > e, 1, 0)

        @when(end, t == A2_FIRST)
        def _():
            get_a()
            for i in range(4):
                a2_copy(i).start()

        first_hops(r)
        in_range(m, n_chunks, multiply)
        job(m, job_multiply)
        in_range(m - lag(LAG_MIDDLE), n_chunks, own_middle)
        job(m - LAG_JOB_MIDDLE, job_middle)
        in_range(m - lag(LAG_FINISH), n_chunks, own_finish)
        job(m - LAG_JOB_FINISH, job_finish)
        last_hops(r)

        extra = t == EXTRA[0]
        for e in EXTRA[1:]:
            extra = extra | (t == e)

        @when(inner, extra)
        def _():
            first_hops(r + 1)
            last_hops(r + 1)

    await_sent(abuf.at[pl.ds(0, 3)], a_snd.at[0])

    def sent(cs):
        await_sent(bbuf.at[pl.ds(0, half), cs], t_snd.at[0])
        await_sent(pbuf.at[:, :, pl.ds(0, hr), cs], r_snd.at[0])
        await_sent(pbuf.at[0, :, pl.ds(0, hr), cs], q_snd.at[0])

    def strip(cs):
        return bbuf.at[pl.ds(0, rows_b), cs]

    @when(inner)
    def _():
        sent(all_cols)
        await_sent(pbuf2.at[:, :, pl.ds(0, hr)], rj_snd.at[0])
        await_sent(pbuf2.at[0, :, pl.ds(0, hr)], qj_snd.at[0])
        await_sent(cbuf, c_snd.at[0])

    @when(z == 0)
    def _():
        await_sent(strip(all_cols), up_snd.at[0])

    @when(z == 3)
    def _():
        await_sent(strip(all_cols), dn_snd.at[0])

    @when(z == 1)
    def _():
        for h in range(2):
            await_sent(strip(all_cols), up_snd.at[h])
        for h in range(3):
            await_sent(strip(rest_cols), dn_snd.at[h])

    @when(z == 2)
    def _():
        for h in range(2):
            await_sent(strip(all_cols), dn_snd.at[h])
        for h in range(3):
            await_sent(strip(rest_cols), up_snd.at[h])

    @when(end)
    def _():
        sent(rest_cols)
        await_sent(abuf, a2_snd.at[0])
        await_got(cbuf, c_rcv.at[0])


def solution(mesh):
    all_axes = ("depth", "row", "col")

    def device_block(a_rows, b_rows):
        rows, depth = a_rows.shape
        rows_b, n_cols = b_rows.shape
        n = n_cols // NC
        hr = rows // 2
        nj = SHARED * NC
        dma = pltpu.SemaphoreType.DMA
        bf16, f32 = jnp.bfloat16, jnp.float32
        return pl.pallas_call(
            functools.partial(kernel, n_cols),
            out_shape=pltpu.VMEM((rows, n_cols), bf16),
            in_specs=[pl.BlockSpec(memory_space=pl.ANY)] * 2,
            out_specs=pl.BlockSpec(memory_space=pltpu.VMEM),
            scratch_shapes=[
                pltpu.VMEM((4, rows, 8 * rows_b), bf16),
                pltpu.VMEM((4, rows, 8 * rows_b), bf16),
                pltpu.VMEM((8 * rows_b, n_cols), bf16),
                pltpu.VMEM((2, 2, rows, n_cols), f32),
                pltpu.VMEM((2, hr, n_cols), f32), pltpu.VMEM((2, hr, n_cols), f32),
                pltpu.VMEM((hr, n_cols), f32), pltpu.VMEM((hr, n_cols), f32),
                pltpu.VMEM((2, 2, rows, nj), f32),
                pltpu.VMEM((2, hr, nj), f32), pltpu.VMEM((2, hr, nj), f32),
                pltpu.VMEM((hr, nj), f32), pltpu.VMEM((hr, nj), f32),
                pltpu.VMEM((rows, nj), bf16),
                dma((3,)), dma((1,)), dma((JOBS,)),
                dma((n,)), dma((n,)), dma((1,)), dma((2, RING_Z)), dma((2, RING_Z)),
                dma((RING,)), dma((RING,)), dma((RING,)), dma((JOBS,)), dma((JOBS,)), dma((1,)),
                dma((1,)), dma((1,)), dma((3,)), dma((3,)),
                dma((1,)), dma((1,)), dma((1,)), dma((1,)), dma((1,)), dma((1,)),
            ],
            compiler_params=pltpu.CompilerParams(collective_id=0, has_side_effects=True, vmem_limit_bytes=56 * 2**20),
            name="product",
        )(a_rows, b_rows)

    return jax.shard_map(device_block, mesh=mesh, in_specs=(P(all_axes, None), P(all_axes, None)), out_specs=P(all_axes, None), check_vma=False)
```

```python
import functools

import jax
import jax.numpy as jnp
from jax import lax
from jax.experimental import pallas as pl
from jax.experimental.pallas import tpu as pltpu
from jax.sharding import PartitionSpec as P

MESH = pl.DeviceIdType.MESH
NC = 256
SHARED = 5
JOBS = 4
FIRST_JOB, JOB_PERIOD = 4, 3
AHEAD = 2
AHEAD_END = 5
A2_FIRST = 3
A2_STEPS = {5: 4, 7: 5, 9: 6, 11: 7}
LAG_MULTIPLY = 1
LAG_MIDDLE, LAG_FINISH = (1, 1), (3, 2)
LAG_JOB_MIDDLE, LAG_JOB_FINISH = 2, 4
RING_Z, RING = 12, 8
EXTRA = (12,)
BACK = 17


def kernel(
    n_cols, a_ref, b_ref, c_ref,
    abuf, abuf2, bbuf, pbuf, rx, ry, sx, sy, pbuf2, rx2, ry2, sx2, sy2, cbuf,
    loc, a_rcv, a2_rcv, up0_rcv, dn0_rcv, out_rcv, up_rcv, dn_rcv, t_rcv, r_rcv, q_rcv, rj_rcv, qj_rcv, c_rcv,
    a_snd, a2_snd, up_snd, dn_snd, t_snd, r_snd, q_snd, rj_snd, qj_snd, c_snd,
):
    depth, y, z = lax.axis_index("depth"), lax.axis_index("row"), lax.axis_index("col")
    x, core = depth // 2, depth % 2
    n_chunks = n_cols // NC
    rows_a = a_ref.shape[0]
    rows_b = b_ref.shape[0]
    half = 4 * rows_b
    hr = rows_a // 2
    jr = rows_a // JOBS
    f32 = jnp.float32
    wide = SHARED * NC

    inner = (z == 1) | (z == 2)
    end = (z == 0) | (z == 3)
    up = (z + 1, y, depth)
    down = (z - 1, y, depth)
    partner = (z + 1 - 2 * (z % 2), y, depth)
    twin = (z, y, 2 * x + 1 - core)
    x_peer = (z, y, 2 * (1 - x) + core)
    y_peer = (z, 1 - y, depth)
    diag = (z, 1 - y, 2 * (1 - x) + core)
    plane = (x_peer, y_peer, diag)
    plane_xy = ((1 - x, y), (x, 1 - y), (1 - x, 1 - y))

    def cols(j):
        return pl.ds(pl.multiple_of(j * NC, NC), NC)

    all_cols = pl.ds(0, n_cols)
    rest_cols = pl.ds(wide, n_cols - wide)

    def shared(j):
        return j < SHARED

    def works(j):
        return inner | ~shared(j)

    def when(*conds):
        both = conds[0]
        for c in conds[1:]:
            both = both & c
        return pl.when(both)

    def b_rows(src):
        return pl.ds(pl.multiple_of(core * half + src * rows_b, rows_b), rows_b)

    def a_cols(px, py, k):
        return pl.ds(pl.multiple_of(((2 * px + k) * 2 + py) * half, half), half)

    load_b = pltpu.make_async_copy(b_ref, bbuf.at[b_rows(z)], loc.at[0])
    load_b.start()
    load_a = []
    for k in range(2):
        load_a.append(pltpu.make_async_copy(a_ref.at[:, a_cols(x, y, k)], abuf.at[2 * x + y, :, pl.ds(k * half, half)], loc.at[1 + k]))
        load_a[-1].start()

    barrier = pltpu.get_barrier_semaphore()
    for peer in plane + (twin,):
        pl.semaphore_signal(barrier, inc=1, device_id=peer, device_id_type=MESH)

    @when(z < 3)
    def _():
        pl.semaphore_signal(barrier, inc=1, device_id=up, device_id_type=MESH)

    @when(z > 0)
    def _():
        pl.semaphore_signal(barrier, inc=1, device_id=down, device_id_type=MESH)

    @when(inner)
    def _():
        pl.semaphore_wait(barrier, 6)

    @when(end)
    def _():
        pl.semaphore_wait(barrier, 5)

    def remote(src, dst, snd, rcv, target):
        return pltpu.make_async_remote_copy(src, dst, snd, rcv, device_id=target, device_id_type=MESH)

    def await_sent(ref, sem):
        remote(ref, ref, sem, loc.at[0], twin).wait_send()

    def await_got(ref, sem):
        remote(ref, ref, loc.at[0], sem, twin).wait_recv()

    def a_copy(i, k):
        px, py = plane_xy[i]
        return remote(a_ref.at[:, a_cols(px, py, k)], abuf.at[2 * x + y, :, pl.ds(k * half, half)], a_snd.at[0], a_rcv.at[0], plane[i])

    def get_a():
        await_got(abuf.at[pl.ds(0, 3)], a_rcv.at[0])

    def job_rows(i):
        return pl.ds(pl.multiple_of(i * jr, jr), jr)

    def a2_copy(i):
        part = jr // 2
        rows = pl.ds(pl.multiple_of(i * part, part), part)
        return remote(abuf.at[:, rows], abuf2.at[:, rows], a2_snd.at[0], a2_rcv.at[i // 2], partner)

    def z_copy(j, src, snd, rcv, target):
        return remote(bbuf.at[b_rows(src), cols(j)], bbuf.at[b_rows(src), cols(j)], snd, rcv, target)

    def up_copy(h, j, src):
        return z_copy(j, src, up_snd.at[h], up0_rcv.at[j] if h == 0 else up_rcv.at[h - 1, j % RING_Z], up)

    def dn_copy(h, j, src):
        return z_copy(j, src, dn_snd.at[h], dn0_rcv.at[j] if h == 0 else dn_rcv.at[h - 1, j % RING_Z], down)

    def outward(src, snd, target):
        return remote(bbuf.at[b_rows(src), rest_cols], bbuf.at[b_rows(src), rest_cols], snd, out_rcv.at[0], target)

    def send_inward(j):
        @when(z < 2)
        def _():
            up_copy(0, j, z).start()

        @when(z > 1)
        def _():
            dn_copy(0, j, z).start()

    def relay(h, j):
        if h == 1:
            @when(inner)
            def _():
                up_copy(0, j, z - 1).wait_recv()

            @when(z == 3, j == SHARED)
            def _():
                outward(z - 1, up_snd.at[0], up).wait_recv()
        else:
            @when(z >= h, (z < 3) | ~shared(j))
            def _():
                up_copy(h - 1, j, z - h).wait_recv()

        if h < 3:
            @when(z >= h, (z < 2) | ((z == 2) & ~shared(j)))
            def _():
                up_copy(h, j, z - h).start()

        if h == 1:
            @when(inner)
            def _():
                dn_copy(0, j, z + 1).wait_recv()

            @when(z == 0, j == SHARED)
            def _():
                outward(z + 1, dn_snd.at[0], down).wait_recv()
        else:
            @when(z <= 3 - h, (z > 0) | ~shared(j))
            def _():
                dn_copy(h - 1, j, z + h).wait_recv()

        if h < 3:
            @when(z <= 3 - h, (z > 1) | ((z == 1) & ~shared(j)))
            def _():
                dn_copy(h, j, z + h).start()

    def twin_copy(j, who):
        rows = pl.ds(pl.multiple_of(who * half, half), half)
        return remote(bbuf.at[rows, cols(j)], bbuf.at[rows, cols(j)], t_snd.at[0], t_rcv.at[j % RING], twin)

    def send_twin(j):
        @when(works(j))
        def _():
            twin_copy(j, core).start()

    def view(own, j):
        if own:
            return pbuf, (rx, ry), (sx, sy), pl.ds(0, hr), pl.ds(hr, hr), pl.ds(0, hr), cols(j)
        lo = pl.multiple_of(j * jr, jr)
        return pbuf2, (rx2, ry2), (sx2, sy2), pl.ds(lo, jr // 2), pl.ds(pl.multiple_of(lo + jr // 2, jr // 2), jr // 2), pl.ds(pl.multiple_of(j * (jr // 2), jr // 2), jr // 2), pl.ds(0, wide)

    def sems(own, j):
        if own:
            return r_snd.at[0], r_rcv.at[j % RING], q_snd.at[0], q_rcv.at[j % RING]
        return rj_snd.at[0], rj_rcv.at[j], qj_snd.at[0], qj_rcv.at[j]

    def first_stage(own, j):
        p, (bx, by), _, low, high, rs, cs = view(own, j)
        snd, rcv, _, _ = sems(own, j)
        remote(p.at[1 - x, :, low, cs], bx.at[:, rs, cs], snd, rcv, x_peer).start()
        remote(p.at[:, 1 - y, high, cs], by.at[:, rs, cs], snd, rcv, y_peer).start()

    def middle(own, j):
        p, (bx, by), (qx, qy), low, high, rs, cs = view(own, j)
        _, got, snd, rcv = sems(own, j)
        await_got(p.at[:, :, low, cs], got)
        p[x, 1 - y, low, cs] += bx[1 - y, rs, cs]
        p[1 - x, y, high, cs] += by[1 - x, rs, cs]
        remote(p.at[x, 1 - y, low, cs], qy.at[rs, cs], snd, rcv, y_peer).start()
        remote(p.at[1 - x, y, high, cs], qx.at[rs, cs], snd, rcv, x_peer).start()

    def finish(own, j):
        p, (bx, by), (qx, qy), low, high, rs, cs = view(own, j)
        out = c_ref if own else cbuf
        await_got(p.at[0, :, low, cs], sems(own, j)[3])
        top = p[x, y, low, cs] + bx[y, rs, cs] + qy[rs, cs]
        bottom = p[x, y, high, cs] + by[x, rs, cs] + qx[rs, cs]
        rows = pl.ds(0, rows_a) if own else job_rows(j)
        out[rows, cs] = jnp.concatenate([top, bottom], axis=0).astype(out.dtype)

    def c_copy(i):
        return remote(cbuf.at[job_rows(i)], c_ref.at[job_rows(i), pl.ds(0, wide)], c_snd.at[0], c_rcv.at[0], partner)

    def multiply(j):
        when(inner, j == 0)(get_a)

        @when(works(j))
        def _():
            twin_copy(j, 1 - core).wait_recv()
            a = abuf[...].reshape(4 * rows_a, 2 * half)
            pbuf[:, :, :, cols(j)] = jnp.dot(a, bbuf[:, cols(j)], preferred_element_type=f32).reshape(2, 2, rows_a, NC)
            first_stage(True, j)

    def own_middle(j):
        when(works(j))(lambda: middle(True, j))

    def own_finish(j):
        @when(works(j))
        def _():
            finish(True, j)

    def job_multiply(i):
        await_got(abuf2.at[:, job_rows(i)], a2_rcv.at[i])
        a = abuf2[:, job_rows(i), :].reshape(4 * jr, 2 * half)

        @pl.loop(0, wide // 256)
        def _(j):
            cs = pl.ds(pl.multiple_of(j * 256, 256), 256)
            pbuf2[:, :, job_rows(i), cs] = jnp.dot(a, bbuf[:, cs], preferred_element_type=f32).reshape(2, 2, jr, 256)

        first_stage(False, i)

    def job_middle(i):
        middle(False, i)

    def job_finish(i):
        finish(False, i)

        @when(i == JOBS - 1)
        def _():
            c_copy(i).start()

    def second_hop(j):
        relay(2, j)
        send_twin(j)

    def third_hop(j):
        relay(3, j)
        send_twin(j)

    def in_range(j, count, fn, *more):
        when((j >= 0) & (j < count), *more)(lambda: fn(j))

    def job(m, fn):
        m = m - FIRST_JOB
        when(inner, m >= 0, m % JOB_PERIOD == 0, m < JOBS * JOB_PERIOD)(lambda: fn(m // JOB_PERIOD))

    for i in range(3):
        for k in range(2):
            a_copy(i, k).start()
    load_b.wait()

    @when(inner)
    def _():
        for j in range(AHEAD):
            send_inward(j)

    @when(end)
    def _():
        @pl.loop(0, AHEAD_END)
        def _(j):
            send_inward(j)

    @when(z == 2)
    def _():
        outward(z, up_snd.at[0], up).start()

    @when(z == 1)
    def _():
        outward(z, dn_snd.at[0], down).start()

    for k in range(2):
        load_a[k].wait()

    flag = (z % 3 + 1) // 2

    def first_hops(r):
        in_range(r + AHEAD, n_chunks, send_inward, inner)
        in_range(r + AHEAD_END, n_chunks, send_inward, end)
        for step, piece in A2_STEPS.items():
            @when(end, r == step)
            def _():
                a2_copy(piece).start()
        in_range(r, n_chunks, functools.partial(relay, 1))
        in_range(r - 1, n_chunks, functools.partial(relay, 2), end)

    def last_hops(r):
        in_range(r - 1, n_chunks, second_hop, inner)
        in_range(r - 2, n_chunks, third_hop, end)

    def lag(pair):
        return pair[1] + flag * (pair[0] - pair[1])

    @pl.loop(0, n_chunks + 2 + LAG_MULTIPLY + max(LAG_FINISH))
    def _(t):
        m = t - 2 - LAG_MULTIPLY + flag
        r = t
        for e in EXTRA:
            r = r + flag * jnp.where(t > e, 1, 0)

        @when(end, t == A2_FIRST)
        def _():
            get_a()
            for i in range(4):
                a2_copy(i).start()

        first_hops(r)
        in_range(m, n_chunks, multiply)
        job(m, job_multiply)
        in_range(m - lag(LAG_MIDDLE), n_chunks, own_middle)
        job(m - LAG_JOB_MIDDLE, job_middle)
        in_range(m - lag(LAG_FINISH), n_chunks, own_finish)
        job(m - LAG_JOB_FINISH, job_finish)
        last_hops(r)

        @when(inner, t == BACK)
        def _():
            for i in range(JOBS - 1):
                c_copy(i).start()

        extra = t == EXTRA[0]
        for e in EXTRA[1:]:
            extra = extra | (t == e)

        @when(inner, extra)
        def _():
            first_hops(r + 1)
            last_hops(r + 1)

    await_sent(abuf.at[pl.ds(0, 3)], a_snd.at[0])

    def sent(cs):
        await_sent(bbuf.at[pl.ds(0, half), cs], t_snd.at[0])
        await_sent(pbuf.at[:, :, pl.ds(0, hr), cs], r_snd.at[0])
        await_sent(pbuf.at[0, :, pl.ds(0, hr), cs], q_snd.at[0])

    def strip(cs):
        return bbuf.at[pl.ds(0, rows_b), cs]

    @when(inner)
    def _():
        sent(all_cols)
        await_sent(pbuf2.at[:, :, pl.ds(0, hr)], rj_snd.at[0])
        await_sent(pbuf2.at[0, :, pl.ds(0, hr)], qj_snd.at[0])
        await_sent(cbuf, c_snd.at[0])

    @when(z == 0)
    def _():
        await_sent(strip(all_cols), up_snd.at[0])

    @when(z == 3)
    def _():
        await_sent(strip(all_cols), dn_snd.at[0])

    @when(z == 1)
    def _():
        for h in range(2):
            await_sent(strip(all_cols), up_snd.at[h])
        for h in range(3):
            await_sent(strip(rest_cols), dn_snd.at[h])

    @when(z == 2)
    def _():
        for h in range(2):
            await_sent(strip(all_cols), dn_snd.at[h])
        for h in range(3):
            await_sent(strip(rest_cols), up_snd.at[h])

    @when(end)
    def _():
        sent(rest_cols)
        await_sent(abuf, a2_snd.at[0])
        await_got(cbuf, c_rcv.at[0])


def solution(mesh):
    all_axes = ("depth", "row", "col")

    def device_block(a_rows, b_rows):
        rows, depth = a_rows.shape
        rows_b, n_cols = b_rows.shape
        n = n_cols // NC
        hr = rows // 2
        nj = SHARED * NC
        dma = pltpu.SemaphoreType.DMA
        bf16, f32 = jnp.bfloat16, jnp.float32
        return pl.pallas_call(
            functools.partial(kernel, n_cols),
            out_shape=pltpu.VMEM((rows, n_cols), bf16),
            in_specs=[pl.BlockSpec(memory_space=pl.ANY)] * 2,
            out_specs=pl.BlockSpec(memory_space=pltpu.VMEM),
            scratch_shapes=[
                pltpu.VMEM((4, rows, 8 * rows_b), bf16),
                pltpu.VMEM((4, rows, 8 * rows_b), bf16),
                pltpu.VMEM((8 * rows_b, n_cols), bf16),
                pltpu.VMEM((2, 2, rows, n_cols), f32),
                pltpu.VMEM((2, hr, n_cols), f32), pltpu.VMEM((2, hr, n_cols), f32),
                pltpu.VMEM((hr, n_cols), f32), pltpu.VMEM((hr, n_cols), f32),
                pltpu.VMEM((2, 2, rows, nj), f32),
                pltpu.VMEM((2, hr, nj), f32), pltpu.VMEM((2, hr, nj), f32),
                pltpu.VMEM((hr, nj), f32), pltpu.VMEM((hr, nj), f32),
                pltpu.VMEM((rows, nj), bf16),
                dma((3,)), dma((1,)), dma((JOBS,)),
                dma((n,)), dma((n,)), dma((1,)), dma((2, RING_Z)), dma((2, RING_Z)),
                dma((RING,)), dma((RING,)), dma((RING,)), dma((JOBS,)), dma((JOBS,)), dma((1,)),
                dma((1,)), dma((1,)), dma((3,)), dma((3,)),
                dma((1,)), dma((1,)), dma((1,)), dma((1,)), dma((1,)), dma((1,)),
            ],
            compiler_params=pltpu.CompilerParams(collective_id=0, has_side_effects=True, vmem_limit_bytes=56 * 2**20),
            name="product",
        )(a_rows, b_rows)

    return jax.shard_map(device_block, mesh=mesh, in_specs=(P(all_axes, None), P(all_axes, None)), out_specs=P(all_axes, None), check_vma=False)
```

```python
import collections
import functools

import jax
import jax.numpy as jnp
from jax import lax
from jax.experimental import pallas as pl
from jax.experimental.pallas import tpu as pltpu
from jax.sharding import PartitionSpec as P

MESH = pl.DeviceIdType.MESH
NC, SMALL = 256, 128
N_SMALL = 0
SHARED = 5
JOBS = 4
FIRST_JOB, JOB_PERIOD = 4, 3
AHEAD = 2
AHEAD_END = 5
A2_FIRST = 3
A2_STEPS = {5: 4, 7: 5, 9: 6, 11: 7}
LAG_MULTIPLY = (1, 1)
LAG_MIDDLE, LAG_FINISH = (1, 1), (3, 3)
LAG_JOB_MIDDLE, LAG_JOB_FINISH = 2, 4
RING_Z, RING = 12, 8
EXTRA = (12,)
BACK = 17

Chunk = collections.namedtuple("Chunk", "j start width")


def n_big(n_cols):
    return (n_cols - N_SMALL * SMALL) // NC


def kernel(
    n_cols, a_ref, b_ref, c_ref,
    abuf, abuf2, bbuf, pbuf, rx, ry, sx, sy, pbuf2, rx2, ry2, sx2, sy2, cbuf,
    loc, a_rcv, a2_rcv, end_rcv, mid_rcv, out_rcv, hop_rcv, t_rcv, r_rcv, q_rcv, rj_rcv, qj_rcv, c_rcv,
    a_snd, a2_snd, up_snd, dn_snd, t_snd, r_snd, q_snd, rj_snd, qj_snd, c_snd,
):
    depth, y, z = lax.axis_index("depth"), lax.axis_index("row"), lax.axis_index("col")
    x, core = depth // 2, depth % 2
    big = n_big(n_cols)
    n_chunks = big + N_SMALL
    rows_a = a_ref.shape[0]
    rows_b = b_ref.shape[0]
    half = 4 * rows_b
    hr = rows_a // 2
    jr = rows_a // JOBS
    f32 = jnp.float32
    wide = SHARED * NC

    inner = (z == 1) | (z == 2)
    end = (z == 0) | (z == 3)
    up = (z + 1, y, depth)
    down = (z - 1, y, depth)
    partner = (z + 1 - 2 * (z % 2), y, depth)
    twin = (z, y, 2 * x + 1 - core)
    x_peer = (z, y, 2 * (1 - x) + core)
    y_peer = (z, 1 - y, depth)
    diag = (z, 1 - y, 2 * (1 - x) + core)
    plane = (x_peer, y_peer, diag)
    plane_xy = ((1 - x, y), (x, 1 - y), (1 - x, 1 - y))

    def big_chunk(j):
        return Chunk(j, j * NC, NC)

    def small_chunk(j):
        return Chunk(j, j * SMALL + big * (NC - SMALL), SMALL)

    def cols(c):
        return pl.ds(pl.multiple_of(c.start, c.width), c.width)

    all_cols = pl.ds(0, n_cols)
    rest_cols = pl.ds(wide, n_cols - wide)

    def shared(j):
        return j < SHARED

    def works(c):
        return inner | ~shared(c.j)

    def when(*conds):
        both = conds[0]
        for c in conds[1:]:
            both = both & c
        return pl.when(both)

    def b_rows(src):
        return pl.ds(pl.multiple_of(core * half + src * rows_b, rows_b), rows_b)

    def a_cols(px, py, k):
        return pl.ds(pl.multiple_of(((2 * px + k) * 2 + py) * half, half), half)

    load_b = pltpu.make_async_copy(b_ref, bbuf.at[b_rows(z)], loc.at[0])
    load_b.start()
    load_a = []
    for k in range(2):
        load_a.append(pltpu.make_async_copy(a_ref.at[:, a_cols(x, y, k)], abuf.at[2 * x + y, :, pl.ds(k * half, half)], loc.at[1 + k]))
        load_a[-1].start()

    barrier = pltpu.get_barrier_semaphore()
    for peer in plane + (twin,):
        pl.semaphore_signal(barrier, inc=1, device_id=peer, device_id_type=MESH)

    @when(z < 3)
    def _():
        pl.semaphore_signal(barrier, inc=1, device_id=up, device_id_type=MESH)

    @when(z > 0)
    def _():
        pl.semaphore_signal(barrier, inc=1, device_id=down, device_id_type=MESH)

    @when(inner)
    def _():
        pl.semaphore_wait(barrier, 6)

    @when(end)
    def _():
        pl.semaphore_wait(barrier, 5)

    def remote(src, dst, snd, rcv, target):
        return pltpu.make_async_remote_copy(src, dst, snd, rcv, device_id=target, device_id_type=MESH)

    def await_sent(ref, sem):
        remote(ref, ref, sem, loc.at[0], twin).wait_send()

    def await_got(ref, sem):
        remote(ref, ref, loc.at[0], sem, twin).wait_recv()

    def a_copy(i, k):
        px, py = plane_xy[i]
        return remote(a_ref.at[:, a_cols(px, py, k)], abuf.at[2 * x + y, :, pl.ds(k * half, half)], a_snd.at[0], a_rcv.at[0], plane[i])

    def get_a():
        await_got(abuf.at[pl.ds(0, 3)], a_rcv.at[0])

    def job_rows(i):
        return pl.ds(pl.multiple_of(i * jr, jr), jr)

    def a2_copy(i):
        part = jr // 2
        rows = pl.ds(pl.multiple_of(i * part, part), part)
        return remote(abuf.at[:, rows], abuf2.at[:, rows], a2_snd.at[0], a2_rcv.at[i // 2], partner)

    def z_copy(c, src, snd, rcv, target):
        return remote(bbuf.at[b_rows(src), cols(c)], bbuf.at[b_rows(src), cols(c)], snd, rcv, target)

    def up_copy(h, c, src, rcv=None):
        return z_copy(c, src, up_snd.at[h], hop_rcv.at[h - 1, c.j % RING_Z] if rcv is None else rcv, up)

    def dn_copy(h, c, src, rcv=None):
        return z_copy(c, src, dn_snd.at[h], hop_rcv.at[h - 1, c.j % RING_Z] if rcv is None else rcv, down)

    def outward(src, snd, target):
        return remote(bbuf.at[b_rows(src), rest_cols], bbuf.at[b_rows(src), rest_cols], snd, out_rcv.at[0], target)

    def send_inward(c):
        @when(z == 0)
        def _():
            up_copy(0, c, z, end_rcv.at[c.j]).start()

        @when(z == 1)
        def _():
            up_copy(0, c, z, mid_rcv.at[c.j % RING_Z]).start()

        @when(z == 2)
        def _():
            dn_copy(0, c, z, mid_rcv.at[c.j % RING_Z]).start()

        @when(z == 3)
        def _():
            dn_copy(0, c, z, end_rcv.at[c.j]).start()

    def first_hop(c):
        @when(z == 1)
        def _():
            dn_copy(0, c, z + 1, mid_rcv.at[c.j % RING_Z]).wait_recv()
            when(~shared(c.j))(lambda: dn_copy(1, c, z + 1).start())
            up_copy(0, c, z - 1, end_rcv.at[c.j]).wait_recv()
            up_copy(1, c, z - 1).start()

        @when(z == 2)
        def _():
            up_copy(0, c, z - 1, mid_rcv.at[c.j % RING_Z]).wait_recv()
            when(~shared(c.j))(lambda: up_copy(1, c, z - 1).start())
            dn_copy(0, c, z + 1, end_rcv.at[c.j]).wait_recv()
            dn_copy(1, c, z + 1).start()

        @when(z == 3, c.j == SHARED)
        def _():
            outward(z - 1, up_snd.at[0], up).wait_recv()

        @when(z == 0, c.j == SHARED)
        def _():
            outward(z + 1, dn_snd.at[0], down).wait_recv()

        when(inner)(lambda: twin_first(c))

    def second_hop(c):
        @when(z == 1)
        def _():
            dn_copy(1, c, z + 2).wait_recv()
            when(~shared(c.j))(lambda: dn_copy(2, c, z + 2).start())

        @when(z == 2)
        def _():
            up_copy(1, c, z - 2).wait_recv()
            when(~shared(c.j))(lambda: up_copy(2, c, z - 2).start())

        when(inner)(lambda: twin_last(c))

        @when(z == 3, ~shared(c.j))
        def _():
            up_copy(1, c, z - 2).wait_recv()
            twin_first(c)

        @when(z == 0, ~shared(c.j))
        def _():
            dn_copy(1, c, z + 2).wait_recv()
            twin_first(c)

    def third_hop(c):
        @when(z == 3, ~shared(c.j))
        def _():
            up_copy(2, c, z - 3).wait_recv()
            twin_last(c)

        @when(z == 0, ~shared(c.j))
        def _():
            dn_copy(2, c, z + 3).wait_recv()
            twin_last(c)

    def twin_part(c, who, start, rows):
        at = pl.ds(pl.multiple_of(who * half + start, rows_b), rows)
        return remote(bbuf.at[at, cols(c)], bbuf.at[at, cols(c)], t_snd.at[0], t_rcv.at[c.j % RING], twin)

    def twin_first(c):
        twin_part(c, core, z // 2 * rows_b, 3 * rows_b).start()

    def twin_last(c):
        twin_part(c, core, (1 - z // 2) * 3 * rows_b, rows_b).start()

    def get_twin(c):
        twin_part(c, 1 - core, 0, half).wait_recv()

    def view(own, j):
        if own:
            return pbuf, (rx, ry), (sx, sy), pl.ds(0, hr), pl.ds(hr, hr), pl.ds(0, hr), cols(j)
        lo = pl.multiple_of(j * jr, jr)
        return pbuf2, (rx2, ry2), (sx2, sy2), pl.ds(lo, jr // 2), pl.ds(pl.multiple_of(lo + jr // 2, jr // 2), jr // 2), pl.ds(pl.multiple_of(j * (jr // 2), jr // 2), jr // 2), pl.ds(0, wide)

    def sems(own, j):
        if own:
            return r_snd.at[0], r_rcv.at[j.j % RING], q_snd.at[0], q_rcv.at[j.j % RING]
        return rj_snd.at[0], rj_rcv.at[j], qj_snd.at[0], qj_rcv.at[j]

    def first_stage(own, j):
        p, (bx, by), _, low, high, rs, cs = view(own, j)
        snd, rcv, _, _ = sems(own, j)
        remote(p.at[1 - x, :, low, cs], bx.at[:, rs, cs], snd, rcv, x_peer).start()
        remote(p.at[:, 1 - y, high, cs], by.at[:, rs, cs], snd, rcv, y_peer).start()

    def middle(own, j):
        p, (bx, by), (qx, qy), low, high, rs, cs = view(own, j)
        _, got, snd, rcv = sems(own, j)
        await_got(p.at[:, :, low, cs], got)
        p[x, 1 - y, low, cs] += bx[1 - y, rs, cs]
        p[1 - x, y, high, cs] += by[1 - x, rs, cs]
        remote(p.at[x, 1 - y, low, cs], qy.at[rs, cs], snd, rcv, y_peer).start()
        remote(p.at[1 - x, y, high, cs], qx.at[rs, cs], snd, rcv, x_peer).start()

    def finish(own, j):
        p, (bx, by), (qx, qy), low, high, rs, cs = view(own, j)
        out = c_ref if own else cbuf
        await_got(p.at[0, :, low, cs], sems(own, j)[3])
        top = p[x, y, low, cs] + bx[y, rs, cs] + qy[rs, cs]
        bottom = p[x, y, high, cs] + by[x, rs, cs] + qx[rs, cs]
        rows = pl.ds(0, rows_a) if own else job_rows(j)
        out[rows, cs] = jnp.concatenate([top, bottom], axis=0).astype(out.dtype)

    def c_copy(i):
        return remote(cbuf.at[job_rows(i)], c_ref.at[job_rows(i), pl.ds(0, wide)], c_snd.at[0], c_rcv.at[0], partner)

    def multiply(c):
        when(inner, c.j == 0)(get_a)

        @when(works(c))
        def _():
            get_twin(c)
            a = abuf[...].reshape(4 * rows_a, 2 * half)
            pbuf[:, :, :, cols(c)] = jnp.dot(a, bbuf[:, cols(c)], preferred_element_type=f32).reshape(2, 2, rows_a, c.width)
            first_stage(True, c)

    def own_middle(c):
        when(works(c))(lambda: middle(True, c))

    def own_finish(c):
        @when(works(c))
        def _():
            finish(True, c)

    def job_multiply(i):
        await_got(abuf2.at[:, job_rows(i)], a2_rcv.at[i])
        a = abuf2[:, job_rows(i), :].reshape(4 * jr, 2 * half)

        @pl.loop(0, wide // 256)
        def _(j):
            cs = pl.ds(pl.multiple_of(j * 256, 256), 256)
            pbuf2[:, :, job_rows(i), cs] = jnp.dot(a, bbuf[:, cs], preferred_element_type=f32).reshape(2, 2, jr, 256)

        first_stage(False, i)

    def job_middle(i):
        middle(False, i)

    def job_finish(i):
        finish(False, i)

        @when(i == JOBS - 1)
        def _():
            c_copy(i).start()

    def in_range(j, fn, *more):
        when((j >= 0) & (j < big), *more)(lambda: fn(big_chunk(j)))
        when((j >= big) & (j < n_chunks), *more)(lambda: fn(small_chunk(j)))

    def job(m, fn):
        m = m - FIRST_JOB
        when(inner, m >= 0, m % JOB_PERIOD == 0, m < JOBS * JOB_PERIOD)(lambda: fn(m // JOB_PERIOD))

    for i in range(3):
        for k in range(2):
            a_copy(i, k).start()
    load_b.wait()

    @when(inner)
    def _():
        for j in range(AHEAD):
            send_inward(big_chunk(j))

    @when(end)
    def _():
        @pl.loop(0, AHEAD_END)
        def _(j):
            send_inward(big_chunk(j))

    @when(z == 2)
    def _():
        outward(z, up_snd.at[0], up).start()

    @when(z == 1)
    def _():
        outward(z, dn_snd.at[0], down).start()

    for k in range(2):
        load_a[k].wait()

    flag = (z % 3 + 1) // 2

    def first_hops(r):
        in_range(r + AHEAD, send_inward, inner)
        in_range(r + AHEAD_END, send_inward, end)
        for step, piece in A2_STEPS.items():
            @when(end, r == step)
            def _():
                a2_copy(piece).start()
        in_range(r, first_hop)
        in_range(r - 1, second_hop, end)

    def last_hops(r):
        in_range(r - 1, second_hop, inner)
        in_range(r - 2, third_hop, end)

    def lag(pair):
        return pair[1] + flag * (pair[0] - pair[1])

    @pl.loop(0, n_chunks + 2 + max(LAG_MULTIPLY) + max(LAG_FINISH))
    def _(t):
        m = t - 2 - lag(LAG_MULTIPLY) + flag
        r = t
        for e in EXTRA:
            r = r + flag * jnp.where(t > e, 1, 0)

        @when(end, t == A2_FIRST)
        def _():
            get_a()
            for i in range(4):
                a2_copy(i).start()

        first_hops(r)
        in_range(m, multiply)
        job(m, job_multiply)
        in_range(m - lag(LAG_MIDDLE), own_middle)
        job(m - LAG_JOB_MIDDLE, job_middle)
        in_range(m - lag(LAG_FINISH), own_finish)
        job(m - LAG_JOB_FINISH, job_finish)
        last_hops(r)

        @when(inner, t == BACK)
        def _():
            for i in range(JOBS - 1):
                c_copy(i).start()

        extra = t == EXTRA[0]
        for e in EXTRA[1:]:
            extra = extra | (t == e)

        @when(inner, extra)
        def _():
            first_hops(r + 1)
            last_hops(r + 1)

    await_sent(abuf.at[pl.ds(0, 3)], a_snd.at[0])

    def sent(cs):
        await_sent(bbuf.at[pl.ds(0, half), cs], t_snd.at[0])
        await_sent(pbuf.at[:, :, pl.ds(0, hr), cs], r_snd.at[0])
        await_sent(pbuf.at[0, :, pl.ds(0, hr), cs], q_snd.at[0])

    def strip(cs):
        return bbuf.at[pl.ds(0, rows_b), cs]

    @when(inner)
    def _():
        sent(all_cols)
        await_sent(pbuf2.at[:, :, pl.ds(0, hr)], rj_snd.at[0])
        await_sent(pbuf2.at[0, :, pl.ds(0, hr)], qj_snd.at[0])
        await_sent(cbuf, c_snd.at[0])

    @when(z == 0)
    def _():
        await_sent(strip(all_cols), up_snd.at[0])

    @when(z == 3)
    def _():
        await_sent(strip(all_cols), dn_snd.at[0])

    @when(z == 1)
    def _():
        for h in range(2):
            await_sent(strip(all_cols), up_snd.at[h])
        for h in range(3):
            await_sent(strip(rest_cols), dn_snd.at[h])

    @when(z == 2)
    def _():
        for h in range(2):
            await_sent(strip(all_cols), dn_snd.at[h])
        for h in range(3):
            await_sent(strip(rest_cols), up_snd.at[h])

    @when(end)
    def _():
        sent(rest_cols)
        await_sent(abuf, a2_snd.at[0])
        await_got(cbuf, c_rcv.at[0])


def solution(mesh):
    all_axes = ("depth", "row", "col")

    def device_block(a_rows, b_rows):
        rows, depth = a_rows.shape
        rows_b, n_cols = b_rows.shape
        n = n_big(n_cols) + N_SMALL
        hr = rows // 2
        nj = SHARED * NC
        dma = pltpu.SemaphoreType.DMA
        bf16, f32 = jnp.bfloat16, jnp.float32
        return pl.pallas_call(
            functools.partial(kernel, n_cols),
            out_shape=pltpu.VMEM((rows, n_cols), bf16),
            in_specs=[pl.BlockSpec(memory_space=pl.ANY)] * 2,
            out_specs=pl.BlockSpec(memory_space=pltpu.VMEM),
            scratch_shapes=[
                pltpu.VMEM((4, rows, 8 * rows_b), bf16),
                pltpu.VMEM((4, rows, 8 * rows_b), bf16),
                pltpu.VMEM((8 * rows_b, n_cols), bf16),
                pltpu.VMEM((2, 2, rows, n_cols), f32),
                pltpu.VMEM((2, hr, n_cols), f32), pltpu.VMEM((2, hr, n_cols), f32),
                pltpu.VMEM((hr, n_cols), f32), pltpu.VMEM((hr, n_cols), f32),
                pltpu.VMEM((2, 2, rows, nj), f32),
                pltpu.VMEM((2, hr, nj), f32), pltpu.VMEM((2, hr, nj), f32),
                pltpu.VMEM((hr, nj), f32), pltpu.VMEM((hr, nj), f32),
                pltpu.VMEM((rows, nj), bf16),
                dma((3,)), dma((1,)), dma((JOBS,)),
                dma((n,)), dma((RING_Z,)), dma((1,)), dma((2, RING_Z)),
                dma((RING,)), dma((RING,)), dma((RING,)), dma((JOBS,)), dma((JOBS,)), dma((1,)),
                dma((1,)), dma((1,)), dma((3,)), dma((3,)),
                dma((1,)), dma((1,)), dma((1,)), dma((1,)), dma((1,)), dma((1,)),
            ],
            compiler_params=pltpu.CompilerParams(collective_id=0, has_side_effects=True, vmem_limit_bytes=56 * 2**20),
            name="product",
        )(a_rows, b_rows)

    return jax.shard_map(device_block, mesh=mesh, in_specs=(P(all_axes, None), P(all_axes, None)), out_specs=P(all_axes, None), check_vma=False)
```

```python
import collections
import functools

import jax
import jax.numpy as jnp
from jax import lax
from jax.experimental import pallas as pl
from jax.experimental.pallas import tpu as pltpu
from jax.sharding import PartitionSpec as P

MESH = pl.DeviceIdType.MESH
NC, SMALL = 256, 128
N_SMALL = 0
HALF = 2
SHARED = 5
JOBS = 4
FIRST_JOB, JOB_PERIOD = 4, 3
AHEAD = 2
AHEAD_END = 5
A2_FIRST, A2_BURST = 3, 4
A2_STEPS = {5: 4, 7: 5, 9: 6, 11: 7}
LAG_MULTIPLY = (1, 1)
LAG_MIDDLE, LAG_FINISH = (1, 1), (3, 3)
LAG_JOB_MIDDLE, LAG_JOB_FINISH = 2, 4
RING_Z, RING = 8, 6
EXTRA = (12,)
BACK = 18

Chunk = collections.namedtuple("Chunk", "j start width")


def n_big(n_cols):
    return (n_cols - N_SMALL * SMALL) // NC


def kernel(
    n_cols, a_ref, b_ref, c_ref,
    abuf, abuf2, bbuf, pbuf, rx, ry, sx, sy, pbuf2, rx2, ry2, sx2, sy2, cbuf,
    loc, a_rcv, a2_rcv, end_rcv, mid_rcv, out_rcv, hop_rcv, t_rcv, r_rcv, q_rcv, rj_rcv, qj_rcv, c_rcv,
    a_snd, a2_snd, up_snd, dn_snd, t_snd, r_snd, q_snd, rj_snd, qj_snd, c_snd,
):
    depth, y, z = lax.axis_index("depth"), lax.axis_index("row"), lax.axis_index("col")
    x, core = depth // 2, depth % 2
    big = n_big(n_cols)
    n_chunks = big + N_SMALL
    rows_a = a_ref.shape[0]
    rows_b = b_ref.shape[0]
    half = 4 * rows_b
    hr = rows_a // 2
    jr = rows_a // JOBS
    f32 = jnp.float32
    wide = SHARED * NC

    inner = (z == 1) | (z == 2)
    end = (z == 0) | (z == 3)
    up = (z + 1, y, depth)
    down = (z - 1, y, depth)
    partner = (z + 1 - 2 * (z % 2), y, depth)
    twin = (z, y, 2 * x + 1 - core)
    x_peer = (z, y, 2 * (1 - x) + core)
    y_peer = (z, 1 - y, depth)
    diag = (z, 1 - y, 2 * (1 - x) + core)
    plane = (x_peer, y_peer, diag)
    plane_xy = ((1 - x, y), (x, 1 - y), (1 - x, 1 - y))

    def big_chunk(j):
        return Chunk(j, j * NC, NC)

    def small_chunk(j):
        return Chunk(j, j * SMALL + big * (NC - SMALL), SMALL)

    def cols(c):
        return pl.ds(pl.multiple_of(c.start, c.width), c.width)

    all_cols = pl.ds(0, n_cols)
    rest_cols = pl.ds(wide, n_cols - wide)

    def shared(j):
        return j < SHARED

    def works(c):
        return inner | ~shared(c.j)

    def when(*conds):
        both = conds[0]
        for c in conds[1:]:
            both = both & c
        return pl.when(both)

    def b_rows(src):
        return pl.ds(pl.multiple_of(core * half + src * rows_b, rows_b), rows_b)

    def a_cols(px, py, k):
        return pl.ds(pl.multiple_of(((2 * px + k) * 2 + py) * half, half), half)

    load_b = pltpu.make_async_copy(b_ref, bbuf.at[b_rows(z)], loc.at[0])
    load_b.start()
    load_a = []
    for k in range(2):
        load_a.append(pltpu.make_async_copy(a_ref.at[:, a_cols(x, y, k)], abuf.at[2 * x + y, :, pl.ds(k * half, half)], loc.at[1 + k]))
        load_a[-1].start()

    barrier = pltpu.get_barrier_semaphore()
    for peer in plane + (twin,):
        pl.semaphore_signal(barrier, inc=1, device_id=peer, device_id_type=MESH)

    @when(z < 3)
    def _():
        pl.semaphore_signal(barrier, inc=1, device_id=up, device_id_type=MESH)

    @when(z > 0)
    def _():
        pl.semaphore_signal(barrier, inc=1, device_id=down, device_id_type=MESH)

    @when(inner)
    def _():
        pl.semaphore_wait(barrier, 6)

    @when(end)
    def _():
        pl.semaphore_wait(barrier, 5)

    def remote(src, dst, snd, rcv, target):
        return pltpu.make_async_remote_copy(src, dst, snd, rcv, device_id=target, device_id_type=MESH)

    def await_sent(ref, sem):
        remote(ref, ref, sem, loc.at[0], twin).wait_send()

    def await_got(ref, sem):
        remote(ref, ref, loc.at[0], sem, twin).wait_recv()

    def a_half(h):
        return pl.ds(h * hr, hr)

    def a_copy(i, k, h):
        px, py = plane_xy[i]
        return remote(a_ref.at[a_half(h), a_cols(px, py, k)], abuf.at[2 * x + y, a_half(h), pl.ds(k * half, half)], a_snd.at[0], a_rcv.at[h], plane[i])

    def get_a(h):
        await_got(abuf.at[pl.ds(0, 3), a_half(h)], a_rcv.at[h])

    def job_rows(i):
        return pl.ds(pl.multiple_of(i * jr, jr), jr)

    def a2_copy(i):
        part = jr // 2
        rows = pl.ds(pl.multiple_of(i * part, part), part)
        return remote(abuf.at[:, rows], abuf2.at[:, rows], a2_snd.at[0], a2_rcv.at[i // 2], partner)

    def z_copy(c, src, snd, rcv, target):
        return remote(bbuf.at[b_rows(src), cols(c)], bbuf.at[b_rows(src), cols(c)], snd, rcv, target)

    def up_copy(h, c, src, rcv=None):
        return z_copy(c, src, up_snd.at[h], hop_rcv.at[h - 1, c.j % RING_Z] if rcv is None else rcv, up)

    def dn_copy(h, c, src, rcv=None):
        return z_copy(c, src, dn_snd.at[h], hop_rcv.at[h - 1, c.j % RING_Z] if rcv is None else rcv, down)

    def outward(src, snd, target):
        return remote(bbuf.at[b_rows(src), rest_cols], bbuf.at[b_rows(src), rest_cols], snd, out_rcv.at[0], target)

    def send_inward(c):
        @when(z == 0)
        def _():
            up_copy(0, c, z, end_rcv.at[c.j]).start()

        @when(z == 1)
        def _():
            up_copy(0, c, z, mid_rcv.at[c.j % RING_Z]).start()

        @when(z == 2)
        def _():
            dn_copy(0, c, z, mid_rcv.at[c.j % RING_Z]).start()

        @when(z == 3)
        def _():
            dn_copy(0, c, z, end_rcv.at[c.j]).start()

    def first_hop(c):
        @when(z == 1)
        def _():
            dn_copy(0, c, z + 1, mid_rcv.at[c.j % RING_Z]).wait_recv()
            when(~shared(c.j))(lambda: dn_copy(1, c, z + 1).start())
            up_copy(0, c, z - 1, end_rcv.at[c.j]).wait_recv()
            up_copy(1, c, z - 1).start()

        @when(z == 2)
        def _():
            up_copy(0, c, z - 1, mid_rcv.at[c.j % RING_Z]).wait_recv()
            when(~shared(c.j))(lambda: up_copy(1, c, z - 1).start())
            dn_copy(0, c, z + 1, end_rcv.at[c.j]).wait_recv()
            dn_copy(1, c, z + 1).start()

        @when(z == 3, c.j == SHARED)
        def _():
            outward(z - 1, up_snd.at[0], up).wait_recv()

        @when(z == 0, c.j == SHARED)
        def _():
            outward(z + 1, dn_snd.at[0], down).wait_recv()

        when(inner)(lambda: twin_first(c))

    def second_hop(c):
        @when(z == 1)
        def _():
            dn_copy(1, c, z + 2).wait_recv()
            when(~shared(c.j))(lambda: dn_copy(2, c, z + 2).start())

        @when(z == 2)
        def _():
            up_copy(1, c, z - 2).wait_recv()
            when(~shared(c.j))(lambda: up_copy(2, c, z - 2).start())

        when(inner)(lambda: twin_last(c))

        @when(z == 3, ~shared(c.j))
        def _():
            up_copy(1, c, z - 2).wait_recv()
            twin_first(c)

        @when(z == 0, ~shared(c.j))
        def _():
            dn_copy(1, c, z + 2).wait_recv()
            twin_first(c)

    def third_hop(c):
        @when(z == 3, ~shared(c.j))
        def _():
            up_copy(2, c, z - 3).wait_recv()
            twin_last(c)

        @when(z == 0, ~shared(c.j))
        def _():
            dn_copy(2, c, z + 3).wait_recv()
            twin_last(c)

    def twin_part(c, who, start, rows):
        at = pl.ds(pl.multiple_of(who * half + start, rows_b), rows)
        return remote(bbuf.at[at, cols(c)], bbuf.at[at, cols(c)], t_snd.at[0], t_rcv.at[c.j % RING], twin)

    def twin_first(c):
        twin_part(c, core, z // 2 * rows_b, 3 * rows_b).start()

    def twin_last(c):
        twin_part(c, core, (1 - z // 2) * 3 * rows_b, rows_b).start()

    def get_twin(c):
        twin_part(c, 1 - core, 0, half).wait_recv()

    def view(own, j):
        if own == HALF:
            q = hr // 2
            return pbuf, (rx, ry), (sx, sy), pl.ds(j * hr, q), pl.ds(j * hr + q, q), pl.ds(j * q, q), pl.ds(0, NC)
        if own:
            return pbuf, (rx, ry), (sx, sy), pl.ds(0, hr), pl.ds(hr, hr), pl.ds(0, hr), cols(j)
        lo = pl.multiple_of(j * jr, jr)
        return pbuf2, (rx2, ry2), (sx2, sy2), pl.ds(lo, jr // 2), pl.ds(pl.multiple_of(lo + jr // 2, jr // 2), jr // 2), pl.ds(pl.multiple_of(j * (jr // 2), jr // 2), jr // 2), pl.ds(0, wide)

    def sems(own, j):
        if own == HALF:
            return r_snd.at[0], r_rcv.at[RING + j], q_snd.at[0], q_rcv.at[RING + j]
        if own:
            return r_snd.at[0], r_rcv.at[j.j % RING], q_snd.at[0], q_rcv.at[j.j % RING]
        return rj_snd.at[0], rj_rcv.at[j], qj_snd.at[0], qj_rcv.at[j]

    def first_stage(own, j):
        p, (bx, by), _, low, high, rs, cs = view(own, j)
        snd, rcv, _, _ = sems(own, j)
        remote(p.at[1 - x, :, low, cs], bx.at[:, rs, cs], snd, rcv, x_peer).start()
        remote(p.at[:, 1 - y, high, cs], by.at[:, rs, cs], snd, rcv, y_peer).start()

    def middle(own, j):
        p, (bx, by), (qx, qy), low, high, rs, cs = view(own, j)
        _, got, snd, rcv = sems(own, j)
        await_got(p.at[:, :, low, cs], got)
        p[x, 1 - y, low, cs] += bx[1 - y, rs, cs]
        p[1 - x, y, high, cs] += by[1 - x, rs, cs]
        remote(p.at[x, 1 - y, low, cs], qy.at[rs, cs], snd, rcv, y_peer).start()
        remote(p.at[1 - x, y, high, cs], qx.at[rs, cs], snd, rcv, x_peer).start()

    def finish(own, j):
        p, (bx, by), (qx, qy), low, high, rs, cs = view(own, j)
        out = c_ref if own else cbuf
        await_got(p.at[0, :, low, cs], sems(own, j)[3])
        top = p[x, y, low, cs] + bx[y, rs, cs] + qy[rs, cs]
        bottom = p[x, y, high, cs] + by[x, rs, cs] + qx[rs, cs]
        rows = a_half(j) if own == HALF else pl.ds(0, rows_a) if own else job_rows(j)
        out[rows, cs] = jnp.concatenate([top, bottom], axis=0).astype(out.dtype)

    def c_copy(i):
        return remote(cbuf.at[job_rows(i)], c_ref.at[job_rows(i), pl.ds(0, wide)], c_snd.at[0], c_rcv.at[0], partner)

    def starts(c):
        return inner & (c.j == 0)

    def multiply(c):
        @when(starts(c))
        def _():
            get_a(0)
            get_twin(c)
            for h in range(2):
                if h == 1:
                    get_a(1)
                a = abuf[:, a_half(h), :].reshape(4 * hr, 2 * half)
                pbuf[:, :, a_half(h), pl.ds(0, NC)] = jnp.dot(a, bbuf[:, pl.ds(0, NC)], preferred_element_type=f32).reshape(2, 2, hr, NC)
                first_stage(HALF, h)

        @when(works(c), ~starts(c))
        def _():
            get_twin(c)
            a = abuf[...].reshape(4 * rows_a, 2 * half)
            pbuf[:, :, :, cols(c)] = jnp.dot(a, bbuf[:, cols(c)], preferred_element_type=f32).reshape(2, 2, rows_a, c.width)
            first_stage(True, c)

    def own_middle(c):
        @when(starts(c))
        def _():
            middle(HALF, 0)
            middle(HALF, 1)

        when(works(c), ~starts(c))(lambda: middle(True, c))

    def own_finish(c):
        @when(starts(c))
        def _():
            finish(HALF, 0)
            finish(HALF, 1)

        when(works(c), ~starts(c))(lambda: finish(True, c))

    def job_multiply(i):
        await_got(abuf2.at[:, job_rows(i)], a2_rcv.at[i])
        a = abuf2[:, job_rows(i), :].reshape(4 * jr, 2 * half)

        @pl.loop(0, wide // 256)
        def _(j):
            cs = pl.ds(pl.multiple_of(j * 256, 256), 256)
            pbuf2[:, :, job_rows(i), cs] = jnp.dot(a, bbuf[:, cs], preferred_element_type=f32).reshape(2, 2, jr, 256)

        first_stage(False, i)

    def job_middle(i):
        middle(False, i)

    def job_finish(i):
        finish(False, i)

        @when(i == JOBS - 1)
        def _():
            c_copy(i).start()

    def in_range(j, fn, *more):
        when((j >= 0) & (j < big), *more)(lambda: fn(big_chunk(j)))
        when((j >= big) & (j < n_chunks), *more)(lambda: fn(small_chunk(j)))

    def job(m, fn):
        m = m - FIRST_JOB
        when(inner, m >= 0, m % JOB_PERIOD == 0, m < JOBS * JOB_PERIOD)(lambda: fn(m // JOB_PERIOD))

    for h in range(2):
        for i in range(3):
            for k in range(2):
                a_copy(i, k, h).start()
    load_b.wait()

    @when(inner)
    def _():
        for j in range(AHEAD):
            send_inward(big_chunk(j))

    @when(end)
    def _():
        @pl.loop(0, AHEAD_END)
        def _(j):
            send_inward(big_chunk(j))

    @when(z == 2)
    def _():
        outward(z, up_snd.at[0], up).start()

    @when(z == 1)
    def _():
        outward(z, dn_snd.at[0], down).start()

    for k in range(2):
        load_a[k].wait()

    flag = (z % 3 + 1) // 2

    def first_hops(r):
        in_range(r + AHEAD, send_inward, inner)
        in_range(r + AHEAD_END, send_inward, end)
        for step, piece in A2_STEPS.items():
            @when(end, r == step)
            def _():
                a2_copy(piece).start()
        in_range(r, first_hop)
        in_range(r - 1, second_hop, end)

    def last_hops(r):
        in_range(r - 1, second_hop, inner)
        in_range(r - 2, third_hop, end)

    def lag(pair):
        return pair[1] + flag * (pair[0] - pair[1])

    @pl.loop(0, n_chunks + 2 + max(LAG_MULTIPLY) + max(LAG_FINISH))
    def _(t):
        m = t - 2 - lag(LAG_MULTIPLY) + flag
        r = t
        for e in EXTRA:
            r = r + flag * jnp.where(t > e, 1, 0)

        @when(end, t == A2_FIRST)
        def _():
            get_a(0)
            get_a(1)
            for i in range(A2_BURST):
                a2_copy(i).start()

        first_hops(r)
        in_range(m, multiply)
        job(m, job_multiply)
        in_range(m - lag(LAG_MIDDLE), own_middle)
        job(m - LAG_JOB_MIDDLE, job_middle)
        in_range(m - lag(LAG_FINISH), own_finish)
        job(m - LAG_JOB_FINISH, job_finish)
        last_hops(r)

        @when(inner, t == BACK)
        def _():
            for i in range(JOBS - 1):
                c_copy(i).start()

        extra = t == EXTRA[0]
        for e in EXTRA[1:]:
            extra = extra | (t == e)

        @when(inner, extra)
        def _():
            first_hops(r + 1)
            last_hops(r + 1)

    await_sent(abuf.at[pl.ds(0, 3)], a_snd.at[0])

    def sent(cs):
        await_sent(bbuf.at[pl.ds(0, half), cs], t_snd.at[0])
        await_sent(pbuf.at[:, :, pl.ds(0, hr), cs], r_snd.at[0])
        await_sent(pbuf.at[0, :, pl.ds(0, hr), cs], q_snd.at[0])

    def strip(cs):
        return bbuf.at[pl.ds(0, rows_b), cs]

    @when(inner)
    def _():
        sent(all_cols)
        await_sent(pbuf2.at[:, :, pl.ds(0, hr)], rj_snd.at[0])
        await_sent(pbuf2.at[0, :, pl.ds(0, hr)], qj_snd.at[0])
        await_sent(cbuf, c_snd.at[0])

    @when(z == 0)
    def _():
        await_sent(strip(all_cols), up_snd.at[0])

    @when(z == 3)
    def _():
        await_sent(strip(all_cols), dn_snd.at[0])

    @when(z == 1)
    def _():
        for h in range(2):
            await_sent(strip(all_cols), up_snd.at[h])
        for h in range(3):
            await_sent(strip(rest_cols), dn_snd.at[h])

    @when(z == 2)
    def _():
        for h in range(2):
            await_sent(strip(all_cols), dn_snd.at[h])
        for h in range(3):
            await_sent(strip(rest_cols), up_snd.at[h])

    @when(end)
    def _():
        sent(rest_cols)
        await_sent(abuf, a2_snd.at[0])
        await_got(cbuf, c_rcv.at[0])


def solution(mesh):
    all_axes = ("depth", "row", "col")

    def device_block(a_rows, b_rows):
        rows, depth = a_rows.shape
        rows_b, n_cols = b_rows.shape
        n = n_big(n_cols) + N_SMALL
        hr = rows // 2
        nj = SHARED * NC
        dma = pltpu.SemaphoreType.DMA
        bf16, f32 = jnp.bfloat16, jnp.float32
        return pl.pallas_call(
            functools.partial(kernel, n_cols),
            out_shape=pltpu.VMEM((rows, n_cols), bf16),
            in_specs=[pl.BlockSpec(memory_space=pl.ANY)] * 2,
            out_specs=pl.BlockSpec(memory_space=pltpu.VMEM),
            scratch_shapes=[
                pltpu.VMEM((4, rows, 8 * rows_b), bf16),
                pltpu.VMEM((4, rows, 8 * rows_b), bf16),
                pltpu.VMEM((8 * rows_b, n_cols), bf16),
                pltpu.VMEM((2, 2, rows, n_cols), f32),
                pltpu.VMEM((2, hr, n_cols), f32), pltpu.VMEM((2, hr, n_cols), f32),
                pltpu.VMEM((hr, n_cols), f32), pltpu.VMEM((hr, n_cols), f32),
                pltpu.VMEM((2, 2, rows, nj), f32),
                pltpu.VMEM((2, hr, nj), f32), pltpu.VMEM((2, hr, nj), f32),
                pltpu.VMEM((hr, nj), f32), pltpu.VMEM((hr, nj), f32),
                pltpu.VMEM((rows, nj), bf16),
                dma((3,)), dma((2,)), dma((JOBS,)),
                dma((n,)), dma((RING_Z,)), dma((1,)), dma((2, RING_Z)),
                dma((RING,)), dma((RING + 2,)), dma((RING + 2,)), dma((JOBS,)), dma((JOBS,)), dma((1,)),
                dma((1,)), dma((1,)), dma((3,)), dma((3,)),
                dma((1,)), dma((1,)), dma((1,)), dma((1,)), dma((1,)), dma((1,)),
            ],
            compiler_params=pltpu.CompilerParams(collective_id=0, has_side_effects=True, vmem_limit_bytes=56 * 2**20),
            name="product",
        )(a_rows, b_rows)

    return jax.shard_map(device_block, mesh=mesh, in_specs=(P(all_axes, None), P(all_axes, None)), out_specs=P(all_axes, None), check_vma=False)
```

```python
import collections
import functools

import jax
import jax.numpy as jnp
from jax import lax
from jax.experimental import pallas as pl
from jax.experimental.pallas import tpu as pltpu
from jax.sharding import PartitionSpec as P

MESH = pl.DeviceIdType.MESH
NC, SMALL = 256, 128
N_SMALL = 0
HALF = 2
SHARED = 5
JOBS = 4
FIRST_JOB, JOB_PERIOD = 4, 3
AHEAD = 2
AHEAD_END = 5
A2_FIRST, A2_BURST = 3, 4
A2_STEPS = {5: 4, 7: 5, 9: 6, 11: 7}
LAG_MULTIPLY = (1, 1)
LAG_MIDDLE, LAG_FINISH = (1, 1), (3, 3)
LAG_JOB_MIDDLE, LAG_JOB_FINISH = 2, 4
RING_Z, RING = 8, 6
EXTRA = (12, 16)
BACK = 18

Chunk = collections.namedtuple("Chunk", "j start width")


def n_big(n_cols):
    return (n_cols - N_SMALL * SMALL) // NC


def kernel(
    n_cols, a_ref, b_ref, c_ref,
    abuf, abuf2, bbuf, pbuf, rx, ry, sx, sy, pbuf2, rx2, ry2, sx2, sy2, cbuf,
    loc, a_rcv, a2_rcv, end_rcv, mid_rcv, out_rcv, hop_rcv, t_rcv, r_rcv, q_rcv, rj_rcv, qj_rcv, c_rcv,
    a_snd, a2_snd, up_snd, dn_snd, t_snd, r_snd, q_snd, rj_snd, qj_snd, c_snd,
):
    depth, y, z = lax.axis_index("depth"), lax.axis_index("row"), lax.axis_index("col")
    x, core = depth // 2, depth % 2
    big = n_big(n_cols)
    n_chunks = big + N_SMALL
    rows_a = a_ref.shape[0]
    rows_b = b_ref.shape[0]
    half = 4 * rows_b
    hr = rows_a // 2
    jr = rows_a // JOBS
    f32 = jnp.float32
    wide = SHARED * NC

    inner = (z == 1) | (z == 2)
    end = (z == 0) | (z == 3)
    up = (z + 1, y, depth)
    down = (z - 1, y, depth)
    partner = (z + 1 - 2 * (z % 2), y, depth)
    twin = (z, y, 2 * x + 1 - core)
    x_peer = (z, y, 2 * (1 - x) + core)
    y_peer = (z, 1 - y, depth)
    diag = (z, 1 - y, 2 * (1 - x) + core)
    plane = (x_peer, y_peer, diag)
    plane_xy = ((1 - x, y), (x, 1 - y), (1 - x, 1 - y))

    def big_chunk(j):
        return Chunk(j, j * NC, NC)

    def small_chunk(j):
        return Chunk(j, j * SMALL + big * (NC - SMALL), SMALL)

    def cols(c):
        return pl.ds(pl.multiple_of(c.start, c.width), c.width)

    all_cols = pl.ds(0, n_cols)
    rest_cols = pl.ds(wide, n_cols - wide)

    def shared(j):
        return j < SHARED

    def works(c):
        return inner | ~shared(c.j)

    def when(*conds):
        both = conds[0]
        for c in conds[1:]:
            both = both & c
        return pl.when(both)

    def b_rows(src):
        return pl.ds(pl.multiple_of(core * half + src * rows_b, rows_b), rows_b)

    def a_cols(px, py, k):
        return pl.ds(pl.multiple_of(((2 * px + k) * 2 + py) * half, half), half)

    load_b = pltpu.make_async_copy(b_ref, bbuf.at[b_rows(z)], loc.at[0])
    load_b.start()
    load_a = []
    for k in range(2):
        load_a.append(pltpu.make_async_copy(a_ref.at[:, a_cols(x, y, k)], abuf.at[2 * x + y, :, pl.ds(k * half, half)], loc.at[1 + k]))
        load_a[-1].start()

    barrier = pltpu.get_barrier_semaphore()
    for peer in plane + (twin,):
        pl.semaphore_signal(barrier, inc=1, device_id=peer, device_id_type=MESH)

    @when(z < 3)
    def _():
        pl.semaphore_signal(barrier, inc=1, device_id=up, device_id_type=MESH)

    @when(z > 0)
    def _():
        pl.semaphore_signal(barrier, inc=1, device_id=down, device_id_type=MESH)

    @when(inner)
    def _():
        pl.semaphore_wait(barrier, 6)

    @when(end)
    def _():
        pl.semaphore_wait(barrier, 5)

    def remote(src, dst, snd, rcv, target):
        return pltpu.make_async_remote_copy(src, dst, snd, rcv, device_id=target, device_id_type=MESH)

    def await_sent(ref, sem):
        remote(ref, ref, sem, loc.at[0], twin).wait_send()

    def await_got(ref, sem):
        remote(ref, ref, loc.at[0], sem, twin).wait_recv()

    def a_half(h):
        return pl.ds(h * hr, hr)

    def a_copy(i, k, h):
        px, py = plane_xy[i]
        return remote(a_ref.at[a_half(h), a_cols(px, py, k)], abuf.at[2 * x + y, a_half(h), pl.ds(k * half, half)], a_snd.at[0], a_rcv.at[h], plane[i])

    def get_a(h):
        await_got(abuf.at[pl.ds(0, 3), a_half(h)], a_rcv.at[h])

    def job_rows(i):
        return pl.ds(pl.multiple_of(i * jr, jr), jr)

    def a2_copy(i):
        part = jr // 2
        rows = pl.ds(pl.multiple_of(i * part, part), part)
        return remote(abuf.at[:, rows], abuf2.at[:, rows], a2_snd.at[0], a2_rcv.at[i // 2], partner)

    def z_copy(c, src, snd, rcv, target):
        return remote(bbuf.at[b_rows(src), cols(c)], bbuf.at[b_rows(src), cols(c)], snd, rcv, target)

    def up_copy(h, c, src, rcv=None):
        return z_copy(c, src, up_snd.at[h], hop_rcv.at[h - 1, c.j % RING_Z] if rcv is None else rcv, up)

    def dn_copy(h, c, src, rcv=None):
        return z_copy(c, src, dn_snd.at[h], hop_rcv.at[h - 1, c.j % RING_Z] if rcv is None else rcv, down)

    def outward(src, snd, target):
        return remote(bbuf.at[b_rows(src), rest_cols], bbuf.at[b_rows(src), rest_cols], snd, out_rcv.at[0], target)

    def send_inward(c):
        @when(z == 0)
        def _():
            up_copy(0, c, z, end_rcv.at[c.j]).start()

        @when(z == 1)
        def _():
            up_copy(0, c, z, mid_rcv.at[c.j % RING_Z]).start()

        @when(z == 2)
        def _():
            dn_copy(0, c, z, mid_rcv.at[c.j % RING_Z]).start()

        @when(z == 3)
        def _():
            dn_copy(0, c, z, end_rcv.at[c.j]).start()

    def first_hop(c):
        @when(z == 1)
        def _():
            dn_copy(0, c, z + 1, mid_rcv.at[c.j % RING_Z]).wait_recv()
            when(~shared(c.j))(lambda: dn_copy(1, c, z + 1).start())
            up_copy(0, c, z - 1, end_rcv.at[c.j]).wait_recv()
            up_copy(1, c, z - 1).start()

        @when(z == 2)
        def _():
            up_copy(0, c, z - 1, mid_rcv.at[c.j % RING_Z]).wait_recv()
            when(~shared(c.j))(lambda: up_copy(1, c, z - 1).start())
            dn_copy(0, c, z + 1, end_rcv.at[c.j]).wait_recv()
            dn_copy(1, c, z + 1).start()

        @when(z == 3, c.j == SHARED)
        def _():
            outward(z - 1, up_snd.at[0], up).wait_recv()

        @when(z == 0, c.j == SHARED)
        def _():
            outward(z + 1, dn_snd.at[0], down).wait_recv()

        when(inner)(lambda: twin_first(c))

    def second_hop(c):
        @when(z == 1)
        def _():
            dn_copy(1, c, z + 2).wait_recv()
            when(~shared(c.j))(lambda: dn_copy(2, c, z + 2).start())

        @when(z == 2)
        def _():
            up_copy(1, c, z - 2).wait_recv()
            when(~shared(c.j))(lambda: up_copy(2, c, z - 2).start())

        when(inner)(lambda: twin_last(c))

        @when(z == 3, ~shared(c.j))
        def _():
            up_copy(1, c, z - 2).wait_recv()
            twin_first(c)

        @when(z == 0, ~shared(c.j))
        def _():
            dn_copy(1, c, z + 2).wait_recv()
            twin_first(c)

    def third_hop(c):
        @when(z == 3, ~shared(c.j))
        def _():
            up_copy(2, c, z - 3).wait_recv()
            twin_last(c)

        @when(z == 0, ~shared(c.j))
        def _():
            dn_copy(2, c, z + 3).wait_recv()
            twin_last(c)

    def twin_part(c, who, start, rows):
        at = pl.ds(pl.multiple_of(who * half + start, rows_b), rows)
        return remote(bbuf.at[at, cols(c)], bbuf.at[at, cols(c)], t_snd.at[0], t_rcv.at[c.j % RING], twin)

    def twin_first(c):
        twin_part(c, core, z // 2 * rows_b, 3 * rows_b).start()

    def twin_last(c):
        twin_part(c, core, (1 - z // 2) * 3 * rows_b, rows_b).start()

    def get_twin(c):
        twin_part(c, 1 - core, 0, half).wait_recv()

    def view(own, j):
        if own == HALF:
            q = hr // 2
            return pbuf, (rx, ry), (sx, sy), pl.ds(j * hr, q), pl.ds(j * hr + q, q), pl.ds(j * q, q), pl.ds(0, NC)
        if own:
            return pbuf, (rx, ry), (sx, sy), pl.ds(0, hr), pl.ds(hr, hr), pl.ds(0, hr), cols(j)
        lo = pl.multiple_of(j * jr, jr)
        return pbuf2, (rx2, ry2), (sx2, sy2), pl.ds(lo, jr // 2), pl.ds(pl.multiple_of(lo + jr // 2, jr // 2), jr // 2), pl.ds(pl.multiple_of(j * (jr // 2), jr // 2), jr // 2), pl.ds(0, wide)

    def sems(own, j):
        if own == HALF:
            return r_snd.at[0], r_rcv.at[RING + j], q_snd.at[0], q_rcv.at[RING + j]
        if own:
            return r_snd.at[0], r_rcv.at[j.j % RING], q_snd.at[0], q_rcv.at[j.j % RING]
        return rj_snd.at[0], rj_rcv.at[j], qj_snd.at[0], qj_rcv.at[j]

    def first_stage(own, j):
        p, (bx, by), _, low, high, rs, cs = view(own, j)
        snd, rcv, _, _ = sems(own, j)
        remote(p.at[1 - x, :, low, cs], bx.at[:, rs, cs], snd, rcv, x_peer).start()
        remote(p.at[:, 1 - y, high, cs], by.at[:, rs, cs], snd, rcv, y_peer).start()

    def middle(own, j):
        p, (bx, by), (qx, qy), low, high, rs, cs = view(own, j)
        _, got, snd, rcv = sems(own, j)
        await_got(p.at[:, :, low, cs], got)
        p[x, 1 - y, low, cs] += bx[1 - y, rs, cs]
        p[1 - x, y, high, cs] += by[1 - x, rs, cs]
        remote(p.at[x, 1 - y, low, cs], qy.at[rs, cs], snd, rcv, y_peer).start()
        remote(p.at[1 - x, y, high, cs], qx.at[rs, cs], snd, rcv, x_peer).start()

    def finish(own, j):
        p, (bx, by), (qx, qy), low, high, rs, cs = view(own, j)
        out = c_ref if own else cbuf
        await_got(p.at[0, :, low, cs], sems(own, j)[3])
        top = p[x, y, low, cs] + bx[y, rs, cs] + qy[rs, cs]
        bottom = p[x, y, high, cs] + by[x, rs, cs] + qx[rs, cs]
        rows = a_half(j) if own == HALF else pl.ds(0, rows_a) if own else job_rows(j)
        out[rows, cs] = jnp.concatenate([top, bottom], axis=0).astype(out.dtype)

    def c_copy(i):
        return remote(cbuf.at[job_rows(i)], c_ref.at[job_rows(i), pl.ds(0, wide)], c_snd.at[0], c_rcv.at[0], partner)

    def starts(c):
        return inner & (c.j == 0)

    def multiply(c):
        @when(starts(c))
        def _():
            get_a(0)
            get_twin(c)
            for h in range(2):
                if h == 1:
                    get_a(1)
                a = abuf[:, a_half(h), :].reshape(4 * hr, 2 * half)
                pbuf[:, :, a_half(h), pl.ds(0, NC)] = jnp.dot(a, bbuf[:, pl.ds(0, NC)], preferred_element_type=f32).reshape(2, 2, hr, NC)
                first_stage(HALF, h)

        @when(works(c), ~starts(c))
        def _():
            get_twin(c)
            a = abuf[...].reshape(4 * rows_a, 2 * half)
            pbuf[:, :, :, cols(c)] = jnp.dot(a, bbuf[:, cols(c)], preferred_element_type=f32).reshape(2, 2, rows_a, c.width)
            first_stage(True, c)

    def own_middle(c):
        @when(starts(c))
        def _():
            middle(HALF, 0)
            middle(HALF, 1)

        when(works(c), ~starts(c))(lambda: middle(True, c))

    def own_finish(c):
        @when(starts(c))
        def _():
            finish(HALF, 0)
            finish(HALF, 1)

        when(works(c), ~starts(c))(lambda: finish(True, c))

    def job_multiply(i):
        await_got(abuf2.at[:, job_rows(i)], a2_rcv.at[i])
        a = abuf2[:, job_rows(i), :].reshape(4 * jr, 2 * half)

        @pl.loop(0, wide // 256)
        def _(j):
            cs = pl.ds(pl.multiple_of(j * 256, 256), 256)
            pbuf2[:, :, job_rows(i), cs] = jnp.dot(a, bbuf[:, cs], preferred_element_type=f32).reshape(2, 2, jr, 256)

        first_stage(False, i)

    def job_middle(i):
        middle(False, i)

    def job_finish(i):
        finish(False, i)

        @when(i == JOBS - 1)
        def _():
            c_copy(i).start()

    def in_range(j, fn, *more):
        when((j >= 0) & (j < big), *more)(lambda: fn(big_chunk(j)))
        when((j >= big) & (j < n_chunks), *more)(lambda: fn(small_chunk(j)))

    def job(m, fn):
        m = m - FIRST_JOB
        when(inner, m >= 0, m % JOB_PERIOD == 0, m < JOBS * JOB_PERIOD)(lambda: fn(m // JOB_PERIOD))

    for i in range(3):
        for k in range(2):
            a_copy(i, k, 0).start()
    load_b.wait()

    @when(inner)
    def _():
        for j in range(AHEAD):
            send_inward(big_chunk(j))

    @when(end)
    def _():
        @pl.loop(0, AHEAD_END)
        def _(j):
            send_inward(big_chunk(j))

    @when(z == 2)
    def _():
        outward(z, up_snd.at[0], up).start()

    @when(z == 1)
    def _():
        outward(z, dn_snd.at[0], down).start()

    for i in range(3):
        for k in range(2):
            a_copy(i, k, 1).start()
    for k in range(2):
        load_a[k].wait()

    flag = (z % 3 + 1) // 2

    def first_hops(r):
        in_range(r + AHEAD, send_inward, inner)
        in_range(r + AHEAD_END, send_inward, end)
        for step, piece in A2_STEPS.items():
            @when(end, r == step)
            def _():
                a2_copy(piece).start()
        in_range(r, first_hop)
        in_range(r - 1, second_hop, end)

    def last_hops(r):
        in_range(r - 1, second_hop, inner)
        in_range(r - 2, third_hop, end)

    def lag(pair):
        return pair[1] + flag * (pair[0] - pair[1])

    @pl.loop(0, n_chunks + 2 + max(LAG_MULTIPLY) + max(LAG_FINISH))
    def _(t):
        m = t - 2 - lag(LAG_MULTIPLY) + flag
        r = t
        for e in EXTRA:
            r = r + flag * jnp.where(t > e, 1, 0)

        @when(end, t == A2_FIRST)
        def _():
            get_a(0)
            get_a(1)
            for i in range(A2_BURST):
                a2_copy(i).start()

        first_hops(r)
        in_range(m, multiply)
        job(m, job_multiply)
        in_range(m - lag(LAG_MIDDLE), own_middle)
        job(m - LAG_JOB_MIDDLE, job_middle)
        in_range(m - lag(LAG_FINISH), own_finish)
        job(m - LAG_JOB_FINISH, job_finish)
        last_hops(r)

        @when(inner, t == BACK)
        def _():
            for i in range(JOBS - 1):
                c_copy(i).start()

        extra = t == EXTRA[0]
        for e in EXTRA[1:]:
            extra = extra | (t == e)

        @when(inner, extra)
        def _():
            first_hops(r + 1)
            last_hops(r + 1)

    await_sent(abuf.at[pl.ds(0, 3)], a_snd.at[0])

    def sent(cs):
        await_sent(bbuf.at[pl.ds(0, half), cs], t_snd.at[0])
        await_sent(pbuf.at[:, :, pl.ds(0, hr), cs], r_snd.at[0])
        await_sent(pbuf.at[0, :, pl.ds(0, hr), cs], q_snd.at[0])

    def strip(cs):
        return bbuf.at[pl.ds(0, rows_b), cs]

    @when(inner)
    def _():
        sent(all_cols)
        await_sent(pbuf2.at[:, :, pl.ds(0, hr)], rj_snd.at[0])
        await_sent(pbuf2.at[0, :, pl.ds(0, hr)], qj_snd.at[0])
        await_sent(cbuf, c_snd.at[0])

    @when(z == 0)
    def _():
        await_sent(strip(all_cols), up_snd.at[0])

    @when(z == 3)
    def _():
        await_sent(strip(all_cols), dn_snd.at[0])

    @when(z == 1)
    def _():
        for h in range(2):
            await_sent(strip(all_cols), up_snd.at[h])
        for h in range(3):
            await_sent(strip(rest_cols), dn_snd.at[h])

    @when(z == 2)
    def _():
        for h in range(2):
            await_sent(strip(all_cols), dn_snd.at[h])
        for h in range(3):
            await_sent(strip(rest_cols), up_snd.at[h])

    @when(end)
    def _():
        sent(rest_cols)
        await_sent(abuf, a2_snd.at[0])
        await_got(cbuf, c_rcv.at[0])


def solution(mesh):
    all_axes = ("depth", "row", "col")

    def device_block(a_rows, b_rows):
        rows, depth = a_rows.shape
        rows_b, n_cols = b_rows.shape
        n = n_big(n_cols) + N_SMALL
        hr = rows // 2
        nj = SHARED * NC
        dma = pltpu.SemaphoreType.DMA
        bf16, f32 = jnp.bfloat16, jnp.float32
        return pl.pallas_call(
            functools.partial(kernel, n_cols),
            out_shape=pltpu.VMEM((rows, n_cols), bf16),
            in_specs=[pl.BlockSpec(memory_space=pl.ANY)] * 2,
            out_specs=pl.BlockSpec(memory_space=pltpu.VMEM),
            scratch_shapes=[
                pltpu.VMEM((4, rows, 8 * rows_b), bf16),
                pltpu.VMEM((4, rows, 8 * rows_b), bf16),
                pltpu.VMEM((8 * rows_b, n_cols), bf16),
                pltpu.VMEM((2, 2, rows, n_cols), f32),
                pltpu.VMEM((2, hr, n_cols), f32), pltpu.VMEM((2, hr, n_cols), f32),
                pltpu.VMEM((hr, n_cols), f32), pltpu.VMEM((hr, n_cols), f32),
                pltpu.VMEM((2, 2, rows, nj), f32),
                pltpu.VMEM((2, hr, nj), f32), pltpu.VMEM((2, hr, nj), f32),
                pltpu.VMEM((hr, nj), f32), pltpu.VMEM((hr, nj), f32),
                pltpu.VMEM((rows, nj), bf16),
                dma((3,)), dma((2,)), dma((JOBS,)),
                dma((n,)), dma((RING_Z,)), dma((1,)), dma((2, RING_Z)),
                dma((RING,)), dma((RING + 2,)), dma((RING + 2,)), dma((JOBS,)), dma((JOBS,)), dma((1,)),
                dma((1,)), dma((1,)), dma((3,)), dma((3,)),
                dma((1,)), dma((1,)), dma((1,)), dma((1,)), dma((1,)), dma((1,)),
            ],
            compiler_params=pltpu.CompilerParams(collective_id=0, has_side_effects=True, vmem_limit_bytes=56 * 2**20),
            name="product",
        )(a_rows, b_rows)

    return jax.shard_map(device_block, mesh=mesh, in_specs=(P(all_axes, None), P(all_axes, None)), out_specs=P(all_axes, None), check_vma=False)
```

```python
import collections
import functools

import jax
import jax.numpy as jnp
from jax import lax
from jax.experimental import pallas as pl
from jax.experimental.pallas import tpu as pltpu
from jax.sharding import PartitionSpec as P

MESH = pl.DeviceIdType.MESH
NC, SMALL = 256, 128
N_SMALL = 0
HALF = 2
SHARED = 5
JOBS = 4
FIRST_JOB, JOB_PERIOD = 4, 3
AHEAD = 2
AHEAD_END = 5
A2_FIRST, A2_BURST = 3, 4
A2_STEPS = {5: 4, 7: 5, 9: 6, 11: 7}
LAG_MULTIPLY = (1, 1)
LAG_MIDDLE, LAG_FINISH = (1, 1), (3, 3)
LAG_JOB_MIDDLE, LAG_JOB_FINISH = 2, 4
RING_Z, RING = 8, 6
EXTRA = (12, 16)
BACK = 18

Chunk = collections.namedtuple("Chunk", "j start width")


def n_big(n_cols):
    return (n_cols - N_SMALL * SMALL) // NC


def kernel(
    n_cols, a_ref, b_ref, c_ref,
    abuf, abuf2, bbuf, pbuf, rx, ry, sx, sy, pbuf2, rx2, ry2, sx2, sy2, cbuf,
    loc, a_rcv, a2_rcv, end_rcv, mid_rcv, out_rcv, hop_rcv, t_rcv, r_rcv, q_rcv, rj_rcv, qj_rcv, c_rcv,
    a_snd, a2_snd, up_snd, dn_snd, t_snd, r_snd, q_snd, rj_snd, qj_snd, c_snd,
):
    depth, y, z = lax.axis_index("depth"), lax.axis_index("row"), lax.axis_index("col")
    x, core = depth // 2, depth % 2
    big = n_big(n_cols)
    n_chunks = big + N_SMALL
    rows_a = a_ref.shape[0]
    rows_b = b_ref.shape[0]
    half = 4 * rows_b
    hr = rows_a // 2
    jr = rows_a // JOBS
    f32 = jnp.float32
    wide = SHARED * NC

    inner = (z == 1) | (z == 2)
    end = (z == 0) | (z == 3)
    up = (z + 1, y, depth)
    down = (z - 1, y, depth)
    partner = (z + 1 - 2 * (z % 2), y, depth)
    twin = (z, y, 2 * x + 1 - core)
    x_peer = (z, y, 2 * (1 - x) + core)
    y_peer = (z, 1 - y, depth)
    diag = (z, 1 - y, 2 * (1 - x) + core)
    plane = (x_peer, y_peer, diag)
    plane_xy = ((1 - x, y), (x, 1 - y), (1 - x, 1 - y))

    def big_chunk(j):
        return Chunk(j, j * NC, NC)

    def small_chunk(j):
        return Chunk(j, j * SMALL + big * (NC - SMALL), SMALL)

    def cols(c):
        return pl.ds(pl.multiple_of(c.start, c.width), c.width)

    all_cols = pl.ds(0, n_cols)
    rest_cols = pl.ds(wide, n_cols - wide)

    def shared(j):
        return j < SHARED

    def works(c):
        return inner | ~shared(c.j)

    def when(*conds):
        both = conds[0]
        for c in conds[1:]:
            both = both & c
        return pl.when(both)

    def b_rows(src):
        return pl.ds(pl.multiple_of(core * half + src * rows_b, rows_b), rows_b)

    def a_cols(px, py, k):
        return pl.ds(pl.multiple_of(((2 * px + k) * 2 + py) * half, half), half)

    load_b = pltpu.make_async_copy(b_ref, bbuf.at[b_rows(z)], loc.at[0])
    load_b.start()
    load_a = []
    for k in range(2):
        load_a.append(pltpu.make_async_copy(a_ref.at[:, a_cols(x, y, k)], abuf.at[2 * x + y, :, pl.ds(k * half, half)], loc.at[1 + k]))
        load_a[-1].start()

    barrier = pltpu.get_barrier_semaphore()
    for peer in plane + (twin,):
        pl.semaphore_signal(barrier, inc=1, device_id=peer, device_id_type=MESH)

    @when(z < 3)
    def _():
        pl.semaphore_signal(barrier, inc=1, device_id=up, device_id_type=MESH)

    @when(z > 0)
    def _():
        pl.semaphore_signal(barrier, inc=1, device_id=down, device_id_type=MESH)

    @when(inner)
    def _():
        pl.semaphore_wait(barrier, 6)

    @when(end)
    def _():
        pl.semaphore_wait(barrier, 5)

    def remote(src, dst, snd, rcv, target):
        return pltpu.make_async_remote_copy(src, dst, snd, rcv, device_id=target, device_id_type=MESH)

    def await_sent(ref, sem):
        remote(ref, ref, sem, loc.at[0], twin).wait_send()

    def await_got(ref, sem):
        remote(ref, ref, loc.at[0], sem, twin).wait_recv()

    def a_half(h):
        return pl.ds(h * hr, hr)

    def a_copy(i, k, h):
        px, py = plane_xy[i]
        return remote(a_ref.at[a_half(h), a_cols(px, py, k)], abuf.at[2 * x + y, a_half(h), pl.ds(k * half, half)], a_snd.at[0], a_rcv.at[h], plane[i])

    def get_a(h):
        await_got(abuf.at[pl.ds(0, 3), a_half(h)], a_rcv.at[h])

    def job_rows(i):
        return pl.ds(pl.multiple_of(i * jr, jr), jr)

    def a2_copy(i):
        part = jr // 2
        rows = pl.ds(pl.multiple_of(i * part, part), part)
        return remote(abuf.at[:, rows], abuf2.at[:, rows], a2_snd.at[0], a2_rcv.at[i // 2], partner)

    def z_copy(c, src, snd, rcv, target):
        return remote(bbuf.at[b_rows(src), cols(c)], bbuf.at[b_rows(src), cols(c)], snd, rcv, target)

    def up_copy(h, c, src, rcv=None):
        return z_copy(c, src, up_snd.at[h], hop_rcv.at[h - 1, c.j % RING_Z] if rcv is None else rcv, up)

    def dn_copy(h, c, src, rcv=None):
        return z_copy(c, src, dn_snd.at[h], hop_rcv.at[h - 1, c.j % RING_Z] if rcv is None else rcv, down)

    def outward(src, snd, target):
        return remote(bbuf.at[b_rows(src), rest_cols], bbuf.at[b_rows(src), rest_cols], snd, out_rcv.at[0], target)

    def send_inward(c):
        @when(z == 0)
        def _():
            up_copy(0, c, z, end_rcv.at[c.j]).start()

        @when(z == 1)
        def _():
            up_copy(0, c, z, mid_rcv.at[c.j % RING_Z]).start()

        @when(z == 2)
        def _():
            dn_copy(0, c, z, mid_rcv.at[c.j % RING_Z]).start()

        @when(z == 3)
        def _():
            dn_copy(0, c, z, end_rcv.at[c.j]).start()

    def first_hop(c):
        @when(z == 1)
        def _():
            dn_copy(0, c, z + 1, mid_rcv.at[c.j % RING_Z]).wait_recv()
            when(~shared(c.j))(lambda: dn_copy(1, c, z + 1).start())
            up_copy(0, c, z - 1, end_rcv.at[c.j]).wait_recv()
            up_copy(1, c, z - 1).start()

        @when(z == 2)
        def _():
            up_copy(0, c, z - 1, mid_rcv.at[c.j % RING_Z]).wait_recv()
            when(~shared(c.j))(lambda: up_copy(1, c, z - 1).start())
            dn_copy(0, c, z + 1, end_rcv.at[c.j]).wait_recv()
            dn_copy(1, c, z + 1).start()

        @when(z == 3, c.j == SHARED)
        def _():
            outward(z - 1, up_snd.at[0], up).wait_recv()

        @when(z == 0, c.j == SHARED)
        def _():
            outward(z + 1, dn_snd.at[0], down).wait_recv()

        when(inner)(lambda: twin_first(c))

    def second_hop(c):
        @when(z == 1)
        def _():
            dn_copy(1, c, z + 2).wait_recv()
            when(~shared(c.j))(lambda: dn_copy(2, c, z + 2).start())

        @when(z == 2)
        def _():
            up_copy(1, c, z - 2).wait_recv()
            when(~shared(c.j))(lambda: up_copy(2, c, z - 2).start())

        when(inner)(lambda: twin_last(c))

        @when(z == 3, ~shared(c.j))
        def _():
            up_copy(1, c, z - 2).wait_recv()
            twin_first(c)

        @when(z == 0, ~shared(c.j))
        def _():
            dn_copy(1, c, z + 2).wait_recv()
            twin_first(c)

    def third_hop(c):
        @when(z == 3, ~shared(c.j))
        def _():
            up_copy(2, c, z - 3).wait_recv()
            twin_last(c)

        @when(z == 0, ~shared(c.j))
        def _():
            dn_copy(2, c, z + 3).wait_recv()
            twin_last(c)

    def twin_part(c, who, start, rows):
        at = pl.ds(pl.multiple_of(who * half + start, rows_b), rows)
        return remote(bbuf.at[at, cols(c)], bbuf.at[at, cols(c)], t_snd.at[0], t_rcv.at[c.j % RING], twin)

    def twin_first(c):
        twin_part(c, core, z // 2 * rows_b, 3 * rows_b).start()

    def twin_last(c):
        twin_part(c, core, (1 - z // 2) * 3 * rows_b, rows_b).start()

    def get_twin(c):
        twin_part(c, 1 - core, 0, half).wait_recv()

    def view(own, j):
        if own == HALF:
            q = hr // 2
            return pbuf, (rx, ry), (sx, sy), pl.ds(j * hr, q), pl.ds(j * hr + q, q), pl.ds(j * q, q), pl.ds(0, NC)
        if own:
            return pbuf, (rx, ry), (sx, sy), pl.ds(0, hr), pl.ds(hr, hr), pl.ds(0, hr), cols(j)
        lo = pl.multiple_of(j * jr, jr)
        return pbuf2, (rx2, ry2), (sx2, sy2), pl.ds(lo, jr // 2), pl.ds(pl.multiple_of(lo + jr // 2, jr // 2), jr // 2), pl.ds(pl.multiple_of(j * (jr // 2), jr // 2), jr // 2), pl.ds(0, wide)

    def sems(own, j):
        if own == HALF:
            return r_snd.at[0], r_rcv.at[RING + j], q_snd.at[0], q_rcv.at[RING + j]
        if own:
            return r_snd.at[0], r_rcv.at[j.j % RING], q_snd.at[0], q_rcv.at[j.j % RING]
        return rj_snd.at[0], rj_rcv.at[j], qj_snd.at[0], qj_rcv.at[j]

    def first_stage(own, j):
        p, (bx, by), _, low, high, rs, cs = view(own, j)
        snd, rcv, _, _ = sems(own, j)
        remote(p.at[1 - x, :, low, cs], bx.at[:, rs, cs], snd, rcv, x_peer).start()
        remote(p.at[:, 1 - y, high, cs], by.at[:, rs, cs], snd, rcv, y_peer).start()

    def middle(own, j):
        p, (bx, by), (qx, qy), low, high, rs, cs = view(own, j)
        _, got, snd, rcv = sems(own, j)
        await_got(p.at[:, :, low, cs], got)
        p[x, 1 - y, low, cs] += bx[1 - y, rs, cs]
        remote(p.at[x, 1 - y, low, cs], qy.at[rs, cs], snd, rcv, y_peer).start()
        p[1 - x, y, high, cs] += by[1 - x, rs, cs]
        remote(p.at[1 - x, y, high, cs], qx.at[rs, cs], snd, rcv, x_peer).start()

    def finish(own, j):
        p, (bx, by), (qx, qy), low, high, rs, cs = view(own, j)
        out = c_ref if own else cbuf
        await_got(p.at[0, :, low, cs], sems(own, j)[3])
        top = p[x, y, low, cs] + bx[y, rs, cs] + qy[rs, cs]
        bottom = p[x, y, high, cs] + by[x, rs, cs] + qx[rs, cs]
        rows = a_half(j) if own == HALF else pl.ds(0, rows_a) if own else job_rows(j)
        out[rows, cs] = jnp.concatenate([top, bottom], axis=0).astype(out.dtype)

    def c_copy(i):
        return remote(cbuf.at[job_rows(i)], c_ref.at[job_rows(i), pl.ds(0, wide)], c_snd.at[0], c_rcv.at[0], partner)

    def starts(c):
        return inner & (c.j == 0)

    def multiply(c):
        @when(starts(c))
        def _():
            get_a(0)
            get_twin(c)
            for h in range(2):
                if h == 1:
                    get_a(1)
                a = abuf[:, a_half(h), :].reshape(4 * hr, 2 * half)
                pbuf[:, :, a_half(h), pl.ds(0, NC)] = jnp.dot(a, bbuf[:, pl.ds(0, NC)], preferred_element_type=f32).reshape(2, 2, hr, NC)
                first_stage(HALF, h)

        @when(works(c), ~starts(c))
        def _():
            get_twin(c)
            a = abuf[...].reshape(4 * rows_a, 2 * half)
            pbuf[:, :, :, cols(c)] = jnp.dot(a, bbuf[:, cols(c)], preferred_element_type=f32).reshape(2, 2, rows_a, c.width)
            first_stage(True, c)

    def own_middle(c):
        @when(starts(c))
        def _():
            middle(HALF, 0)
            middle(HALF, 1)

        when(works(c), ~starts(c))(lambda: middle(True, c))

    def own_finish(c):
        @when(starts(c))
        def _():
            finish(HALF, 0)
            finish(HALF, 1)

        when(works(c), ~starts(c))(lambda: finish(True, c))

    def job_multiply(i):
        await_got(abuf2.at[:, job_rows(i)], a2_rcv.at[i])
        a = abuf2[:, job_rows(i), :].reshape(4 * jr, 2 * half)

        @pl.loop(0, wide // 256)
        def _(j):
            cs = pl.ds(pl.multiple_of(j * 256, 256), 256)
            pbuf2[:, :, job_rows(i), cs] = jnp.dot(a, bbuf[:, cs], preferred_element_type=f32).reshape(2, 2, jr, 256)

        first_stage(False, i)

    def job_middle(i):
        middle(False, i)

    def job_finish(i):
        finish(False, i)

        @when(i == JOBS - 1)
        def _():
            c_copy(i).start()

    def in_range(j, fn, *more):
        when((j >= 0) & (j < big), *more)(lambda: fn(big_chunk(j)))
        when((j >= big) & (j < n_chunks), *more)(lambda: fn(small_chunk(j)))

    def job(m, fn):
        m = m - FIRST_JOB
        when(inner, m >= 0, m % JOB_PERIOD == 0, m < JOBS * JOB_PERIOD)(lambda: fn(m // JOB_PERIOD))

    for i in range(3):
        for k in range(2):
            a_copy(i, k, 0).start()
    load_b.wait()

    @when(inner)
    def _():
        for j in range(AHEAD):
            send_inward(big_chunk(j))

    @when(end)
    def _():
        @pl.loop(0, AHEAD_END)
        def _(j):
            send_inward(big_chunk(j))

    @when(z == 2)
    def _():
        outward(z, up_snd.at[0], up).start()

    @when(z == 1)
    def _():
        outward(z, dn_snd.at[0], down).start()

    for i in range(3):
        for k in range(2):
            a_copy(i, k, 1).start()
    for k in range(2):
        load_a[k].wait()

    flag = (z % 3 + 1) // 2

    def first_hops(r):
        in_range(r + AHEAD, send_inward, inner)
        in_range(r + AHEAD_END, send_inward, end)
        for step, piece in A2_STEPS.items():
            @when(end, r == step)
            def _():
                a2_copy(piece).start()
        in_range(r, first_hop)
        in_range(r - 1, second_hop, end)

    def last_hops(r):
        in_range(r - 1, second_hop, inner)
        in_range(r - 2, third_hop, end)

    def lag(pair):
        return pair[1] + flag * (pair[0] - pair[1])

    @pl.loop(0, n_chunks + 2 + max(LAG_MULTIPLY) + max(LAG_FINISH))
    def _(t):
        m = t - 2 - lag(LAG_MULTIPLY) + flag
        r = t
        for e in EXTRA:
            r = r + flag * jnp.where(t > e, 1, 0)

        @when(end, t == A2_FIRST)
        def _():
            get_a(0)
            get_a(1)
            for i in range(A2_BURST):
                a2_copy(i).start()

        first_hops(r)
        in_range(m, multiply)
        job(m, job_multiply)
        in_range(m - lag(LAG_MIDDLE), own_middle)
        job(m - LAG_JOB_MIDDLE, job_middle)
        in_range(m - lag(LAG_FINISH), own_finish)
        job(m - LAG_JOB_FINISH, job_finish)
        last_hops(r)

        @when(inner, t == BACK)
        def _():
            for i in range(JOBS - 1):
                c_copy(i).start()

        extra = t == EXTRA[0]
        for e in EXTRA[1:]:
            extra = extra | (t == e)

        @when(inner, extra)
        def _():
            first_hops(r + 1)
            last_hops(r + 1)

    await_sent(abuf.at[pl.ds(0, 3)], a_snd.at[0])

    def sent(cs):
        await_sent(bbuf.at[pl.ds(0, half), cs], t_snd.at[0])
        await_sent(pbuf.at[:, :, pl.ds(0, hr), cs], r_snd.at[0])
        await_sent(pbuf.at[0, :, pl.ds(0, hr), cs], q_snd.at[0])

    def strip(cs):
        return bbuf.at[pl.ds(0, rows_b), cs]

    @when(inner)
    def _():
        sent(all_cols)
        await_sent(pbuf2.at[:, :, pl.ds(0, hr)], rj_snd.at[0])
        await_sent(pbuf2.at[0, :, pl.ds(0, hr)], qj_snd.at[0])
        await_sent(cbuf, c_snd.at[0])

    @when(z == 0)
    def _():
        await_sent(strip(all_cols), up_snd.at[0])

    @when(z == 3)
    def _():
        await_sent(strip(all_cols), dn_snd.at[0])

    @when(z == 1)
    def _():
        for h in range(2):
            await_sent(strip(all_cols), up_snd.at[h])
        for h in range(3):
            await_sent(strip(rest_cols), dn_snd.at[h])

    @when(z == 2)
    def _():
        for h in range(2):
            await_sent(strip(all_cols), dn_snd.at[h])
        for h in range(3):
            await_sent(strip(rest_cols), up_snd.at[h])

    @when(end)
    def _():
        sent(rest_cols)
        await_sent(abuf, a2_snd.at[0])
        await_got(cbuf, c_rcv.at[0])


def solution(mesh):
    all_axes = ("depth", "row", "col")

    def device_block(a_rows, b_rows):
        rows, depth = a_rows.shape
        rows_b, n_cols = b_rows.shape
        n = n_big(n_cols) + N_SMALL
        hr = rows // 2
        nj = SHARED * NC
        dma = pltpu.SemaphoreType.DMA
        bf16, f32 = jnp.bfloat16, jnp.float32
        return pl.pallas_call(
            functools.partial(kernel, n_cols),
            out_shape=pltpu.VMEM((rows, n_cols), bf16),
            in_specs=[pl.BlockSpec(memory_space=pl.ANY)] * 2,
            out_specs=pl.BlockSpec(memory_space=pltpu.VMEM),
            scratch_shapes=[
                pltpu.VMEM((4, rows, 8 * rows_b), bf16),
                pltpu.VMEM((4, rows, 8 * rows_b), bf16),
                pltpu.VMEM((8 * rows_b, n_cols), bf16),
                pltpu.VMEM((2, 2, rows, n_cols), f32),
                pltpu.VMEM((2, hr, n_cols), f32), pltpu.VMEM((2, hr, n_cols), f32),
                pltpu.VMEM((hr, n_cols), f32), pltpu.VMEM((hr, n_cols), f32),
                pltpu.VMEM((2, 2, rows, nj), f32),
                pltpu.VMEM((2, hr, nj), f32), pltpu.VMEM((2, hr, nj), f32),
                pltpu.VMEM((hr, nj), f32), pltpu.VMEM((hr, nj), f32),
                pltpu.VMEM((rows, nj), bf16),
                dma((3,)), dma((2,)), dma((JOBS,)),
                dma((n,)), dma((RING_Z,)), dma((1,)), dma((2, RING_Z)),
                dma((RING,)), dma((RING + 2,)), dma((RING + 2,)), dma((JOBS,)), dma((JOBS,)), dma((1,)),
                dma((1,)), dma((1,)), dma((3,)), dma((3,)),
                dma((1,)), dma((1,)), dma((1,)), dma((1,)), dma((1,)), dma((1,)),
            ],
            compiler_params=pltpu.CompilerParams(collective_id=0, has_side_effects=True, vmem_limit_bytes=56 * 2**20),
            name="product",
        )(a_rows, b_rows)

    return jax.shard_map(device_block, mesh=mesh, in_specs=(P(all_axes, None), P(all_axes, None)), out_specs=P(all_axes, None), check_vma=False)
```
